32 devices in a mesh: section: 4 (over y, core), dp: 8 (over z, x).
Axes of the slice: x: 2, y: 2, z: 4, core: 2. Of those that a mesh axis runs over, the one named last changes fastest.
Arguments:
- inputs: bfloat16 [1536, 4096], P('dp'), may hold values from -6 to 6
- output_cotangent: bfloat16 [1536, 4096], P('dp'), may hold values from -6 to 6
- lengths: int32 [16], P('dp'), may hold values from 24 to 96
- query_examples: int32 [16], replicated, may hold values from 0 to 15
- norm_gain: bfloat16 [4, 4096], P('section'), may hold values from 0.5 to 1.5
- value_weight: bfloat16 [4, 4096, 1024], P('section', 'dp'), may hold values from -0.09375 to 0.09375
- output_weight: bfloat16 [4, 4096, 1024], P('section', 'dp'), may hold values from -0.1875 to 0.1875
- input_projection: bfloat16 [4, 32, 4096], P('section'), may hold values from -0.09375 to 0.09375
- output_projection: bfloat16 [4, 32, 1024], P('section'), may hold values from -0.1875 to 0.1875
- fisher_prior: float32 [4, 1024, 1024], P('section'), as said below
Outputs:
- scores: float32 [16, 16], P('dp')
The draws below stay inside these ranges and needn't reach their ends.
Inputs may be any that keep to these rules, and one draw needn't show every extreme that they name: `fisher_prior`: each block's 1024 x 1024 matrix is symmetric and positive definite.
All inputs are finite; a program needn't handle non-finite values.
Results may differ from the reference program's by a relative error of at most 0.0013.
Values may be sent and summed in bfloat16 or wider, within the bound.
A program may use at most 128 MiB of HBM per device.

```python
import math
import jax
import jax.numpy as jnp
from jax import lax

D = 4096
KV = 1024
RI = 32
RO = 32
LEN = 96
QUERIES = 16
SECTIONS = 4
EXAMPLES = 16
TOKENS = 1536
K = 1024


def draw_fisher_prior(key, part):
    factor_key, diagonal_key = jax.random.split(key, 2)
    factors = jax.random.normal(factor_key, (SECTIONS, K, K), jnp.float32)
    shared = jnp.einsum('sij,skj->sik', factors, factors, precision=lax.Precision.HIGHEST) / K
    spread = jnp.exp(jax.random.uniform(diagonal_key, (SECTIONS, K), jnp.float32, math.log(0.5), math.log(4.0)))
    prior_matrix = shared + spread[:, :, None] * jnp.eye(K, dtype=jnp.float32)[None]
    return prior_matrix


def plant(entries, rng, low, high):
    index_at = [jax.random.randint(jax.random.fold_in(rng, axis), (), 0, length) for axis, length in enumerate(entries.shape)]
    longest = entries.shape.index(max(entries.shape))
    beside = index_at[:longest] + [(index_at[longest] + 1) % entries.shape[longest]] + index_at[longest + 1:]
    return entries.at[tuple(index_at)].set(low).at[tuple(beside)].set(high)


def shard_levels(stream_key, shape, cuts, least, largest):
    level, own = 1.0, jax.random.fold_in(stream_key, 6)
    for axis_at, shards_of in cuts:
        draws = jnp.exp(jax.random.uniform(jax.random.fold_in(own, axis_at), (shards_of,), jnp.float32, least / len(cuts), largest / len(cuts)))
        level = level * jnp.repeat(draws, shape[axis_at] // shards_of).reshape([-1 if axis == axis_at else 1 for axis in range(len(shape))])
    return level


def centred(rng, shape, width, most, pieces=(), kind=jnp.bfloat16):
    entries = jax.random.normal(rng, shape, jnp.float32) * width
    if len(pieces) > 0:
        entries = shard_levels(rng, shape, pieces, -0.22, 0.18) * entries
    return jnp.clip(entries, min=-most, max=most).astype(kind)


def setup_inputs(seed: int = 0) -> dict:
    splits = jax.random.split(jax.random.key(seed), 11)
    inputs = centred(splits[0], (TOKENS, D), 1.0, 6.0, ((0, 8),))
    output_cotangent = centred(splits[1], (TOKENS, D), 1.0, 6.0, ((0, 8),))
    lengths = plant(jax.random.randint(splits[2], (EXAMPLES,), LEN // 4, LEN + 1), jax.random.fold_in(splits[2], 1), LEN // 4, LEN).astype(jnp.int32)
    query_examples = plant(jax.random.randint(splits[3], (QUERIES,), 0, EXAMPLES), jax.random.fold_in(splits[3], 1), 0, EXAMPLES - 1).astype(jnp.int32)
    norm_gain = jnp.clip(1.0 + 0.1 * jax.random.normal(splits[4], (SECTIONS, D), jnp.float32), 0.5, 1.5).astype(jnp.bfloat16)
    value_weight = centred(splits[5], (SECTIONS, D, KV), D ** -0.5, 0.09375, ((0, 4), (1, 8)))
    output_weight = centred(splits[6], (SECTIONS, D, KV), KV ** -0.5, 0.1875, ((0, 4), (1, 8)))
    input_projection = centred(splits[7], (SECTIONS, RI, D), D ** -0.5, 0.09375, ((0, 4),))
    output_projection = centred(splits[8], (SECTIONS, RO, KV), KV ** -0.5, 0.1875, ((0, 4),))
    fisher_prior = draw_fisher_prior(jax.random.fold_in(splits[10], 71), 0)
    return dict(inputs=inputs, output_cotangent=output_cotangent, lengths=lengths, query_examples=query_examples, norm_gain=norm_gain, value_weight=value_weight, output_weight=output_weight, input_projection=input_projection, output_projection=output_projection, fisher_prior=fisher_prior)


def normalize(hidden, gain):
    widened = hidden.astype(jnp.float32)
    factor = lax.rsqrt(lax.optimization_barrier(jnp.mean(widened * widened, axis=-1, keepdims=True)) + 1e-05)
    return (widened * factor * gain.astype(jnp.float32)).astype(jnp.bfloat16)

def forward_block(hidden, gain, value_map, output_map, input_map):
    normed = normalize(hidden, gain)
    values = jnp.dot(normed.astype(jnp.float32), value_map.astype(jnp.float32), preferred_element_type=jnp.float32)
    activated = jax.nn.silu(values).astype(jnp.bfloat16)
    branch = lax.dot_general(activated.astype(jnp.float32), output_map.astype(jnp.float32), (((1,), (1,)), ((), ())), preferred_element_type=jnp.float32)
    following = (hidden.astype(jnp.float32) + branch).astype(jnp.bfloat16)
    features = lax.dot_general(normed.astype(jnp.float32), input_map.astype(jnp.float32), (((1,), (1,)), ((), ())), preferred_element_type=jnp.float32).astype(jnp.bfloat16)
    return (following, values, features)

def backward_block(hidden, values, cotangent, gain, value_map, output_map, output_map_small):
    widened = hidden.astype(jnp.float32)
    factor = lax.rsqrt(lax.optimization_barrier(jnp.mean(widened * widened, axis=-1, keepdims=True)) + 1e-05)
    upstream = jnp.dot(cotangent.astype(jnp.float32), output_map.astype(jnp.float32), preferred_element_type=jnp.float32)
    logistic = jax.nn.sigmoid(values)
    slopes = (upstream * logistic * (1.0 + values * (1.0 - logistic))).astype(jnp.bfloat16)
    signals = lax.dot_general(slopes.astype(jnp.float32), output_map_small.astype(jnp.float32), (((1,), (1,)), ((), ())), preferred_element_type=jnp.float32).astype(jnp.bfloat16)
    normed_grad = lax.dot_general(slopes.astype(jnp.float32), value_map.astype(jnp.float32), (((1,), (1,)), ((), ())), preferred_element_type=jnp.float32)
    weighted = normed_grad * gain.astype(jnp.float32)
    inner_mean = lax.optimization_barrier(jnp.mean(weighted * widened, axis=-1, keepdims=True))
    hidden_grad = factor * weighted - widened * (factor * factor * factor) * inner_mean
    previous = (cotangent.astype(jnp.float32) + hidden_grad).astype(jnp.bfloat16)
    return (previous, signals)

def reference(inputs, output_cotangent, lengths, query_examples, norm_gain, value_weight, output_weight, input_projection, output_projection, fisher_prior):
    positions = jnp.arange(LEN, dtype=jnp.int32)
    keep = (positions[None, :] < lengths[:, None]).astype(jnp.bfloat16)
    hidden = inputs
    stored_hidden = []
    stored_values = []
    stored_features = []
    for section in range(SECTIONS):
        stored_hidden.append(hidden)
        hidden, values, features = forward_block(hidden, norm_gain[section], value_weight[section], output_weight[section], input_projection[section])
        stored_values.append(values)
        stored_features.append(features)
    cotangent = (output_cotangent.reshape(EXAMPLES, LEN, D) * keep[:, :, None]).reshape(TOKENS, D)
    scores = jnp.zeros((EXAMPLES, QUERIES), jnp.float32)
    for section in reversed(range(SECTIONS)):
        cotangent, signals = backward_block(stored_hidden[section], stored_values[section], cotangent, norm_gain[section], value_weight[section], output_weight[section], output_projection[section])
        grads = jnp.einsum('elo,eli->eoi', signals.reshape(EXAMPLES, LEN, RO).astype(jnp.float32), stored_features[section].reshape(EXAMPLES, LEN, RI).astype(jnp.float32), precision=lax.Precision.HIGHEST) / LEN
        flat = grads.reshape(EXAMPLES, K)
        fisher = jnp.dot(flat.T, flat, precision=lax.Precision.HIGHEST)
        hessian = fisher_prior[section] + fisher
        chosen = flat[query_examples]
        lower_factor = jnp.linalg.cholesky(hessian)
        solved = jax.scipy.linalg.cho_solve((lower_factor, True), chosen.T)
        scores = scores + jnp.dot(flat, solved, precision=lax.Precision.HIGHEST)
    return scores
```

```python
import functools

import jax
import jax.numpy as jnp
from jax import lax
from jax.experimental import pallas as pl
from jax.experimental.pallas import tpu as pltpu
from jax.sharding import PartitionSpec as P


HIGHEST = lax.Precision.HIGHEST


def inverted(block):
    size = block.shape[0]
    rows = lax.broadcasted_iota(jnp.int32, block.shape, 0)
    columns = lax.broadcasted_iota(jnp.int32, block.shape, 1)

    def sweep(pivot, held):
        at_row, at_column = rows == pivot, columns == pivot
        row = jnp.sum(jnp.where(at_row, held, 0.0), axis=0, keepdims=True)
        column = jnp.sum(jnp.where(at_column, held, 0.0), axis=1, keepdims=True)
        corner = jnp.sum(jnp.where(at_column[:1], row, 0.0), axis=1, keepdims=True)
        scale = 1.0 / corner
        scaled = row * scale
        updated = held - column * scaled
        updated = jnp.where(at_row, scaled, updated)
        updated = jnp.where(at_column, column * scale, updated)
        return jnp.where(at_row & at_column, -scale, updated)

    return -lax.fori_loop(0, size, sweep, block)


def sweep_strip(work, strip, step, block):
    span = pl.ds(pl.multiple_of(step * block, block), block)
    corner = inverted(work[span, span])
    strip[...] = jnp.dot(
        corner, work[span, :], precision=HIGHEST, preferred_element_type=jnp.float32
    )
    strip[:, span] = -corner


def sweep_rest(work, strip, step, block):
    span = pl.ds(pl.multiple_of(step * block, block), block)

    @pl.loop(0, work.shape[0] // block)
    def _(other):
        across = pl.ds(pl.multiple_of(other * block, block), block)

        @pl.when(other != step)
        def _():
            work[across, :] -= jnp.dot(
                work[span, across].T, strip[...], precision=HIGHEST,
                preferred_element_type=jnp.float32,
            )
            work[across, span] = strip[:, across].T

    work[span, :] = strip[...]


MESH = pl.DeviceIdType.MESH
CONTRACT_LAST = (((1,), (1,)), ((), ()))
PAIR = 2
PIECES = 4
BLOCK = 128
LANES = 128


def flipped(device, bit):
    return device + (1 - 2 * lax.rem(lax.div(device, bit), 2)) * bit


def mate(device, mask):
    bit = 1
    while bit <= mask:
        if mask & bit:
            device = flipped(device, bit)
        bit *= 2
    return device


def slot_of(device):
    return lax.div(device, 2 * PAIR) * PAIR + lax.rem(device, PAIR)


def gather_events(count):
    bits = []
    bit = count // 2
    while bit >= 1:
        if bit != PAIR:
            bits.append(bit)
        bit //= 2
    held, events = [0], []
    for bit in bits:
        events += [(bit, mask) for mask in held]
        held += [mask | bit for mask in held]
    return events


def span(index, size):
    return pl.ds(pl.multiple_of(index * size, size), size)


def window_kernel(
    sections, count,
    inputs, targets, gain, value_shard, output_shard, input_map, output_map_small, prior, queries,
    scores,
    weights, work, strip, hidden, following, cotangent, previous, values, upstream, normed,
    activated, features, factors, squares, gain_half, input_half, first_out, first_in,
    extra_out, extra_in, second_out, second_in, flats, everyone, rows_all, final,
    gather_send, gather_receive, own_weights, prior_done, entry_own, entry_send, entry_receive,
    forward_send, forward_receive, backward_send, backward_receive,
    first_send, first_receive, extra_send, extra_receive, second_send, second_receive,
    publish_send, publish_receive, final_send, final_receive,
):
    section, me = lax.axis_index("section"), lax.axis_index("dp")
    has_before, has_after = section > 0, section < sections - 1
    before, after = lax.max(section - 1, 0), lax.min(section + 1, sections - 1)
    side = lax.rem(lax.div(me, PAIR), 2)
    partner = flipped(me, PAIR)
    batches, length, width = inputs.shape
    entries = 2 * batches
    half, value_width = weights.shape[1], weights.shape[2]
    rows = value_shard.shape[0]
    piece_rows = rows // PIECES
    stretch = PAIR * rows
    stretches = half // stretch
    size = work.shape[0]
    blocks = size // BLOCK
    feature_width = input_map.shape[0]
    signal_width = output_map_small.shape[0]
    chunks = forward_send.shape[1]
    chunk = half // chunks
    tiles = first_send.shape[1]
    tile = value_width // tiles
    group = 16
    shards = (value_shard, output_shard)
    value_map, output_map = weights.at[0], weights.at[1]
    events = gather_events(count)

    def gather_copy(number, array, piece, first):
        bit, mask = events[number]
        at = slot_of(mate(me, mask)) * PIECES + piece
        there = weights.at[array, span(at, piece_rows), :]
        here = shards[array].at[span(piece, piece_rows), :] if first else there
        return pltpu.make_async_remote_copy(
            src_ref=here,
            dst_ref=there,
            send_sem=gather_send.at[number, array, piece],
            recv_sem=gather_receive.at[number, array, piece],
            device_id={"dp": flipped(me, bit)},
            device_id_type=MESH,
        )

    def serve(array, piece):
        for number, (bit, mask) in enumerate(events):
            forwards = [later for later, (_, want) in enumerate(events) if want == bit | mask]
            if forwards:
                gather_copy(number, array, piece, False).wait_recv()
            for later in forwards:
                gather_copy(later, array, piece, False).start()

    def collect(array):
        for number, (bit, mask) in enumerate(events):
            if all(want != bit | mask for _, want in events):
                @pl.loop(0, PIECES)
                def _(piece):
                    gather_copy(number, array, piece, False).wait_recv()

        kept[array].wait()

    def entry_copy(kind, entry, part, remote):
        source = (inputs, targets)[kind]
        sink = (hidden, cotangent)[kind]
        wanted = 1 - side if remote else side
        here = source.at[entry, :, span(2 * part + wanted, stretch)]
        there = sink.at[side * batches + entry, :, span(part, stretch)]
        if not remote:
            return pltpu.make_async_copy(here, there, entry_own.at[kind, entry, part])
        return pltpu.make_async_remote_copy(
            src_ref=here,
            dst_ref=there,
            send_sem=entry_send.at[kind, entry, part],
            recv_sem=entry_receive.at[kind, entry, part],
            device_id={"dp": partner},
            device_id_type=MESH,
        )

    def entry_wait(kind, batch):
        sink = (hidden, cotangent)[kind]
        owner, entry = lax.div(batch, batches), lax.rem(batch, batches)
        for part in range(stretches):
            there = sink.at[batch, :, span(part, stretch)]

            @pl.when(owner == side)
            def _():
                pltpu.make_async_copy(there, there, entry_own.at[kind, entry, part]).wait()

            @pl.when(owner != side)
            def _():
                pltpu.make_async_remote_copy(
                    src_ref=there,
                    dst_ref=there,
                    send_sem=entry_send.at[kind, entry, part],
                    recv_sem=entry_receive.at[kind, entry, part],
                    device_id={"dp": partner},
                    device_id_type=MESH,
                ).wait_recv()

    def hop(source, sink, send, receive, device, batch, piece):
        columns = span(piece, chunk)
        return pltpu.make_async_remote_copy(
            src_ref=source.at[batch, :, columns],
            dst_ref=sink.at[batch, :, columns],
            send_sem=send.at[batch, piece],
            recv_sem=receive.at[batch, piece],
            device_id={"section": device},
            device_id_type=MESH,
        )

    def forward_copy(batch, piece):
        return hop(following, hidden, forward_send, forward_receive, after, batch, piece)

    def backward_copy(batch, piece):
        return hop(previous, cotangent, backward_send, backward_receive, before, batch, piece)

    def swap(source, sink, send, receive, batch, at):
        columns = span(at, tile)
        return pltpu.make_async_remote_copy(
            src_ref=source.at[batch, :, columns],
            dst_ref=sink.at[batch, :, columns],
            send_sem=send.at[batch, at],
            recv_sem=receive.at[batch, at],
            device_id={"dp": partner},
            device_id_type=MESH,
        )

    def first_copy(batch, at):
        return swap(first_out, first_in, first_send, first_receive, batch, at)

    def second_copy(batch, at):
        return swap(second_out, second_in, second_send, second_receive, batch, at)

    def extra_copy(batch):
        return pltpu.make_async_remote_copy(
            src_ref=extra_out.at[batch],
            dst_ref=extra_in.at[batch],
            send_sem=extra_send.at[batch],
            recv_sem=extra_receive.at[batch],
            device_id={"dp": partner},
            device_id_type=MESH,
        )

    def invert_step(step):
        sweep_strip(work, strip, step, BLOCK)
        sweep_rest(work, strip, step, BLOCK)

    prior_copy = pltpu.make_async_copy(prior, work, prior_done)
    prior_copy.start()
    mine = span(slot_of(me), rows)
    kept = [
        pltpu.make_async_copy(shards[array], weights.at[array, mine, :], own_weights.at[array])
        for array in range(2)
    ]
    barrier = pltpu.get_barrier_semaphore()

    @pl.loop(1, count)
    def _(offset):
        pl.semaphore_signal(
            barrier, inc=1, device_id={"dp": lax.rem(me + offset, count)}, device_id_type=MESH
        )

    @pl.loop(1, sections)
    def _(offset):
        pl.semaphore_signal(
            barrier, inc=1, device_id={"section": lax.rem(section + offset, sections)},
            device_id_type=MESH,
        )

    pl.semaphore_wait(barrier, count + sections - 2)

    for kind, wanted in ((0, jnp.logical_not(has_before)), (1, jnp.logical_not(has_after))):
        @pl.when(wanted)
        def _():
            for entry in range(batches):
                for part in range(stretches):
                    entry_copy(kind, entry, part, True).start()
                    entry_copy(kind, entry, part, False).start()

    for array in range(2):
        for piece in range(PIECES):
            for number, (_, mask) in enumerate(events):
                if mask == 0:
                    gather_copy(number, array, piece, True).start()
    for copy in kept:
        copy.start()

    input_half[...] = jnp.zeros_like(input_half)
    for part in range(stretches):
        there = pl.ds(part * stretch, stretch)
        here = span(2 * part + side, stretch)
        gain_half[:, there] = gain[:, here]
        input_half[:feature_width, there] = input_map[:, here]
    prior_copy.wait()

    early = min(blocks, PIECES)
    rest = blocks - early

    @pl.loop(0, PIECES)
    def _(step):
        @pl.when(step < early)
        def _():
            sweep_strip(work, strip, step, BLOCK)

        first = 2 * step
        serve(lax.div(first, PIECES), lax.rem(first, PIECES))

        @pl.when(step < early)
        def _():
            sweep_rest(work, strip, step, BLOCK)

        second = first + 1
        serve(lax.div(second, PIECES), lax.rem(second, PIECES))

    collect(0)
    edge = lax.div(rest * section, 2 * max(sections - 1, 1))

    @pl.loop(early, early + edge)
    def _(step):
        invert_step(step)

    @pl.loop(0, entries)
    def _(batch):
        @pl.when(has_before)
        def _():
            @pl.loop(0, chunks)
            def _(piece):
                forward_copy(batch, piece).wait_recv()

        @pl.when(jnp.logical_not(has_before))
        def _():
            entry_wait(0, batch)

        @pl.loop(0, length // group)
        def _(at):
            part = span(at, group)
            widened = hidden[batch, part, :].astype(jnp.float32)
            squares[part, :] = jnp.sum(widened * widened, axis=-1, keepdims=True)
            normed[part, :] = (widened * gain_half[...]).astype(jnp.bfloat16)

        extras = lax.dot_general(
            normed[...], input_half[...], CONTRACT_LAST, preferred_element_type=jnp.float32
        )
        lanes = lax.broadcasted_iota(jnp.int32, extras.shape, 1)
        extra_out[batch] = jnp.where(lanes == feature_width, squares[...], extras)
        extra_copy(batch).start()

        @pl.loop(0, tiles)
        def _(at):
            columns = span(at, tile)
            found = jnp.dot(
                normed[...], value_map[:, columns], preferred_element_type=jnp.float32
            )
            values[batch, :, columns] = found
            first_out[batch, :, columns] = found.astype(jnp.bfloat16)
            first_copy(batch, at).start()

        extra_copy(batch).wait_recv()
        both = extra_out[batch] + extra_in[batch]
        total = both[:, feature_width : feature_width + 1]
        factor = lax.rsqrt(total * (1.0 / width) + 1e-05)
        factors[batch] = factor
        features[batch] = (both[:, :feature_width] * factor).astype(jnp.bfloat16)

        @pl.loop(0, tiles)
        def _(at):
            columns = span(at, tile)
            first_copy(batch, at).wait_recv()
            partial = first_in[batch, :, columns].astype(jnp.float32)
            found = (values[batch, :, columns] + partial) * factors[batch]
            values[batch, :, columns] = found
            activated[:, columns] = (found / (1.0 + jnp.exp(-found))).astype(jnp.bfloat16)

        @pl.when(batch == 0)
        def _():
            collect(1)

        @pl.when(has_after)
        def _():
            @pl.loop(0, chunks)
            def _(piece):
                columns = span(piece, chunk)
                branch = lax.dot_general(
                    activated[...], output_map[columns, :], CONTRACT_LAST,
                    preferred_element_type=jnp.float32,
                )
                following[batch, :, columns] = (
                    hidden[batch, :, columns].astype(jnp.float32) + branch
                ).astype(jnp.bfloat16)
                forward_copy(batch, piece).start()

    @pl.loop(early + edge, blocks - edge)
    def _(step):
        invert_step(step)

    @pl.loop(0, entries)
    def _(batch):
        @pl.when(has_after)
        def _():
            @pl.loop(0, chunks)
            def _(piece):
                backward_copy(batch, piece).wait_recv()

        @pl.when(jnp.logical_not(has_after))
        def _():
            entry_wait(1, batch)

        @pl.loop(0, tiles)
        def _(at):
            columns = span(at, tile)
            found = jnp.dot(
                cotangent[batch], output_map[:, columns], preferred_element_type=jnp.float32
            )
            upstream[:, columns] = found
            second_out[batch, :, columns] = found.astype(jnp.bfloat16)
            second_copy(batch, at).start()

        slopes = activated

        def slope_tile(at, total):
            columns = span(at, tile)
            second_copy(batch, at).wait_recv()
            arrived = upstream[:, columns] + second_in[batch, :, columns].astype(jnp.float32)
            found = values[batch, :, columns]
            logistic = 1.0 / (1.0 + jnp.exp(-found))
            slope = (arrived * logistic * (1.0 + found * (1.0 - logistic))).astype(jnp.bfloat16)
            slopes[:, columns] = slope
            return total + jnp.sum(slope.astype(jnp.float32) * found, axis=-1, keepdims=True)

        total = lax.fori_loop(0, tiles, slope_tile, jnp.zeros((length, 1), jnp.float32))
        factor = factors[batch]
        shrink = total * (factor * factor) * (1.0 / width)

        @pl.when(has_before)
        def _():
            @pl.loop(0, chunks)
            def _(piece):
                columns = span(piece, chunk)
                normed_grad = lax.dot_general(
                    slopes[...], value_map[columns, :], CONTRACT_LAST,
                    preferred_element_type=jnp.float32,
                )
                weighted = normed_grad * gain_half[:, columns]
                hidden_grad = (
                    factor * weighted - hidden[batch, :, columns].astype(jnp.float32) * shrink
                )
                previous[batch, :, columns] = (
                    cotangent[batch, :, columns].astype(jnp.float32) + hidden_grad
                ).astype(jnp.bfloat16)
                backward_copy(batch, piece).start()

        signals = lax.dot_general(
            slopes[...], output_map_small[...], CONTRACT_LAST, preferred_element_type=jnp.float32
        ).astype(jnp.bfloat16)
        shape = (signal_width, size)
        entry = lax.broadcasted_iota(jnp.int32, shape, 1)
        line = lax.broadcasted_iota(jnp.int32, shape, 0)
        outer = jnp.where(lax.div(entry, feature_width) == line, 1.0, 0.0).astype(jnp.bfloat16)
        shape = (feature_width, size)
        entry = lax.broadcasted_iota(jnp.int32, shape, 1)
        line = lax.broadcasted_iota(jnp.int32, shape, 0)
        inner = jnp.where(lax.rem(entry, feature_width) == line, 1.0, 0.0).astype(jnp.bfloat16)
        left = jnp.dot(signals, outer, preferred_element_type=jnp.float32)
        right = jnp.dot(features[batch], inner, preferred_element_type=jnp.float32)
        flat = jnp.sum(left * right, axis=0, keepdims=True) * (1.0 / length)
        flats[lax.div(batch, batches), pl.ds(lax.rem(batch, batches), 1), :] = flat

    @pl.loop(blocks - edge, blocks)
    def _(step):
        invert_step(step)

    everyone[me] = flats[side]

    def publish(offset, origin):
        return pltpu.make_async_remote_copy(
            src_ref=everyone.at[origin],
            dst_ref=everyone.at[origin],
            send_sem=publish_send.at[offset],
            recv_sem=publish_receive.at[offset],
            device_id={"dp": lax.rem(me + offset, count)},
            device_id_type=MESH,
        )

    @pl.loop(1, count)
    def _(offset):
        publish(offset, me).start()

    @pl.loop(1, count)
    def _(offset):
        publish(offset, lax.rem(me + count - offset, count)).wait_recv()

    for device in range(count):
        rows_all[device * batches : (device + 1) * batches, :] = everyone[device]
    grads = rows_all[...]
    examples = count * batches
    product = jnp.dot(grads, work[...], precision=HIGHEST, preferred_element_type=jnp.float32)
    gram = -lax.dot_general(
        product, grads, CONTRACT_LAST, precision=HIGHEST, preferred_element_type=jnp.float32
    )
    shape = (examples, examples)
    diagonal = lax.broadcasted_iota(jnp.int32, shape, 0) == lax.broadcasted_iota(jnp.int32, shape, 1)
    inverse = inverted(gram + jnp.where(diagonal, 1.0, 0.0))
    picked = lax.broadcasted_iota(jnp.int32, (8, examples), 0)
    columns = lax.broadcasted_iota(jnp.int32, (8, examples), 1)
    pick = jnp.where((columns == me * batches + picked) & (picked < batches), 1.0, 0.0)
    owners = lax.broadcasted_iota(jnp.int32, (examples, queries.shape[1]), 0)
    selector = jnp.where(owners == queries[...], 1.0, 0.0)
    ours = jnp.dot(pick, gram, precision=HIGHEST, preferred_element_type=jnp.float32)
    chosen = jnp.dot(inverse, selector, precision=HIGHEST, preferred_element_type=jnp.float32)
    final[section] = jnp.dot(ours, chosen, precision=HIGHEST, preferred_element_type=jnp.float32)

    def finish(offset, origin):
        return pltpu.make_async_remote_copy(
            src_ref=final.at[origin],
            dst_ref=final.at[origin],
            send_sem=final_send.at[offset],
            recv_sem=final_receive.at[offset],
            device_id={"section": lax.rem(section + offset, sections)},
            device_id_type=MESH,
        )

    @pl.loop(1, sections)
    def _(offset):
        finish(offset, section).start()

    @pl.loop(1, sections)
    def _(offset):
        finish(offset, lax.rem(section + sections - offset, sections)).wait_recv()

    result = final[0]
    for other in range(1, sections):
        result = result + final[other]
    scores[...] = result[: scores.shape[0], : scores.shape[1]]

    @pl.loop(1, sections)
    def _(offset):
        finish(offset, section).wait_send()

    @pl.loop(1, count)
    def _(offset):
        publish(offset, me).wait_send()

    for kind, wanted in ((0, jnp.logical_not(has_before)), (1, jnp.logical_not(has_after))):
        @pl.when(wanted)
        def _():
            for entry in range(batches):
                for part in range(stretches):
                    entry_copy(kind, entry, part, True).wait_send()

    for number, (_, mask) in enumerate(events):
        for array in range(2):
            @pl.loop(0, PIECES)
            def _(piece):
                gather_copy(number, array, piece, mask == 0).wait_send()

    @pl.loop(0, entries)
    def _(batch):
        extra_copy(batch).wait_send()

        @pl.loop(0, tiles)
        def _(at):
            first_copy(batch, at).wait_send()
            second_copy(batch, at).wait_send()

        @pl.loop(0, chunks)
        def _(piece):
            @pl.when(has_after)
            def _():
                forward_copy(batch, piece).wait_send()

            @pl.when(has_before)
            def _():
                backward_copy(batch, piece).wait_send()


def window(
    inputs, targets, gain, value_shard, output_shard, input_map, output_map_small, prior, queries
):
    sections, count = lax.axis_size("section"), lax.axis_size("dp")
    batches, length, width = inputs.shape
    rows, value_width = value_shard.shape
    entries = 2 * batches
    half = width // 2
    size = prior.shape[0]
    feature_width = input_map.shape[0]
    asked = queries.shape[0]
    padded = jnp.full((1, LANES * pl.cdiv(asked, LANES)), -1, jnp.int32)
    padded = lax.dynamic_update_slice(padded, queries[None, :], (0, 0))
    chunks, tiles = 8, 4
    events = len(gather_events(count))
    stretches = half // (PAIR * rows)
    dma = pltpu.SemaphoreType.DMA
    stream = pltpu.VMEM((entries, length, half), jnp.bfloat16)
    parts = pltpu.VMEM((entries, length, value_width), jnp.bfloat16)
    extra = pltpu.VMEM((entries, length, LANES), jnp.float32)
    anywhere = pl.BlockSpec(memory_space=pl.ANY)
    inside = pl.BlockSpec(memory_space=pltpu.VMEM)
    return pl.pallas_call(
        functools.partial(window_kernel, sections, count),
        out_shape=jax.ShapeDtypeStruct((batches, asked), jnp.float32),
        in_specs=[
            anywhere, anywhere, inside, anywhere, anywhere, inside, inside, anywhere, inside
        ],
        out_specs=inside,
        scratch_shapes=[
            pltpu.VMEM((2, half, value_width), jnp.bfloat16),
            pltpu.VMEM((size, size), jnp.float32),
            pltpu.VMEM((BLOCK, size), jnp.float32),
            stream, stream, stream, stream,
            pltpu.VMEM((entries, length, value_width), jnp.float32),
            pltpu.VMEM((length, value_width), jnp.float32),
            pltpu.VMEM((length, half), jnp.bfloat16),
            pltpu.VMEM((length, value_width), jnp.bfloat16),
            pltpu.VMEM((entries, length, feature_width), jnp.bfloat16),
            pltpu.VMEM((entries, length, 1), jnp.float32),
            pltpu.VMEM((length, 1), jnp.float32),
            pltpu.VMEM((1, half), jnp.float32),
            pltpu.VMEM((LANES, half), jnp.bfloat16),
            parts, parts, extra, extra, parts, parts,
            pltpu.VMEM((2, batches, size), jnp.float32),
            pltpu.VMEM((count, batches, size), jnp.float32),
            pltpu.VMEM((count * batches, size), jnp.float32),
            pltpu.VMEM((sections, 8, padded.shape[1]), jnp.float32),
            dma((events, 2, PIECES)), dma((events, 2, PIECES)), dma((2,)), dma,
            dma((2, batches, stretches)), dma((2, batches, stretches)),
            dma((2, batches, stretches)),
            dma((entries, chunks)), dma((entries, chunks)),
            dma((entries, chunks)), dma((entries, chunks)),
            dma((entries, tiles)), dma((entries, tiles)), dma((entries,)), dma((entries,)),
            dma((entries, tiles)), dma((entries, tiles)),
            dma((count,)), dma((count,)), dma((sections,)), dma((sections,)),
        ],
        compiler_params=pltpu.CompilerParams(
            collective_id=1, has_side_effects=True, vmem_limit_bytes=52 * 2**20
        ),
        name="window",
    )(
        inputs, targets, gain, value_shard, output_shard, input_map, output_map_small, prior,
        padded,
    )


def per_device(
    inputs,
    output_cotangent,
    lengths,
    query_examples,
    norm_gain,
    value_weight,
    output_weight,
    input_projection,
    output_projection,
    fisher_prior,
):
    batches = lengths.shape[0]
    example_rows = inputs.shape[0] // batches
    width = inputs.shape[1]
    positions = jnp.arange(example_rows, dtype=jnp.int32)
    keep = (positions[None, :] < lengths[:, None]).astype(jnp.bfloat16)
    targets = output_cotangent.reshape(batches, example_rows, width) * keep[:, :, None]
    return window(
        inputs.reshape(batches, example_rows, width), targets, norm_gain.astype(jnp.float32),
        value_weight[0], output_weight[0], input_projection[0], output_projection[0],
        fisher_prior[0], query_examples,
    )


def solution(mesh):
    placed = (
        P("dp", None),
        P("dp", None),
        P("dp"),
        P(),
        P("section", None),
        P("section", "dp", None),
        P("section", "dp", None),
        P("section", None, None),
        P("section", None, None),
        P("section", None, None),
    )
    return jax.shard_map(
        per_device, mesh=mesh, in_specs=placed, out_specs=P("dp", None), check_vma=False
    )
```

```python
import functools

import jax
import jax.numpy as jnp
from jax import lax
from jax.experimental import pallas as pl
from jax.experimental.pallas import tpu as pltpu
from jax.sharding import PartitionSpec as P


HIGHEST = lax.Precision.HIGHEST


GROUP = 8


def small_inverse(held):
    count = len(held)
    held = [list(line) for line in held]
    for pivot in range(count):
        scale = 1.0 / held[pivot][pivot]
        line = list(held[pivot])
        scaled = [value * scale for value in line]
        for i in range(count):
            for j in range(i, count):
                if i != pivot and j != pivot:
                    held[i][j] = held[j][i] = held[i][j] - line[i] * scaled[j]
        for j in range(count):
            held[pivot][j] = held[j][pivot] = scaled[j]
        held[pivot][pivot] = -scale
    return [[-value for value in line] for line in held]


def sweep_square(square):
    rows, columns = square.shape
    lanes = lax.broadcasted_iota(jnp.int32, (GROUP, columns), 1)
    lines = lax.broadcasted_iota(jnp.int32, (GROUP, columns), 0)
    wide = lax.broadcasted_iota(jnp.int32, (rows, columns), 1)

    @pl.loop(0, rows // GROUP)
    def _(at):
        base = at * GROUP
        part = pl.ds(pl.multiple_of(base, GROUP), GROUP)
        panel = square[part, :]
        corner = [
            jnp.sum(jnp.where(lanes == base + k, panel, 0.0), axis=1, keepdims=True)
            for k in range(GROUP)
        ]
        spread = [
            [jnp.broadcast_to(corner[k][i : i + 1, :], (1, columns)) for k in range(GROUP)]
            for i in range(GROUP)
        ]
        inverse = small_inverse(spread)
        inside = (lanes >= base) & (lanes < base + GROUP)
        unit = jnp.where(lanes - base == lines, 1.0, 0.0)
        source = jnp.where(inside, unit, panel)
        built = []
        for i in range(GROUP):
            total = inverse[i][0] * source[:1, :]
            for k in range(1, GROUP):
                total = total + inverse[i][k] * source[k : k + 1, :]
            built.append(total)
        strip = jnp.concatenate(built, axis=0)
        signed = jnp.where(inside, -strip, strip)
        full = square[...]
        within = (wide >= base) & (wide < base + GROUP)
        updated = jnp.where(within, 0.0, full)
        for k in range(GROUP):
            column = jnp.sum(jnp.where(wide == base + k, full, 0.0), axis=1, keepdims=True)
            updated = updated - column * signed[k : k + 1, :]
        square[...] = updated
        square[part, :] = signed


def sweep_strip(work, strip, square, step, block):
    part = pl.ds(pl.multiple_of(step * block, block), block)
    square[...] = work[part, part]
    sweep_square(square)
    corner = square[...]
    strip[...] = -jnp.dot(
        corner, work[part, :], precision=HIGHEST, preferred_element_type=jnp.float32
    )
    strip[:, part] = corner


def sweep_rest(work, strip, step, block):
    span = pl.ds(pl.multiple_of(step * block, block), block)

    @pl.loop(0, work.shape[0] // block)
    def _(other):
        across = pl.ds(pl.multiple_of(other * block, block), block)

        @pl.when(other != step)
        def _():
            work[across, :] -= jnp.dot(
                work[span, across].T, strip[...], precision=HIGHEST,
                preferred_element_type=jnp.float32,
            )
            work[across, span] = strip[:, across].T

    work[span, :] = strip[...]


MESH = pl.DeviceIdType.MESH
CONTRACT_LAST = (((1,), (1,)), ((), ()))
PAIR = 2
PIECES = 4
BLOCK = 128
LANES = 128


def flipped(device, bit):
    return device + (1 - 2 * lax.rem(lax.div(device, bit), 2)) * bit


def mate(device, mask):
    bit = 1
    while bit <= mask:
        if mask & bit:
            device = flipped(device, bit)
        bit *= 2
    return device


def slot_of(device):
    return lax.div(device, 2 * PAIR) * PAIR + lax.rem(device, PAIR)


def gather_events(count):
    bits = []
    bit = count // 2
    while bit >= 1:
        if bit != PAIR:
            bits.append(bit)
        bit //= 2
    held, events = [0], []
    for bit in bits:
        events += [(bit, mask) for mask in held]
        held += [mask | bit for mask in held]
    return events


def span(index, size):
    return pl.ds(pl.multiple_of(index * size, size), size)


def window_kernel(
    sections, count,
    inputs, targets, gain, value_shard, output_shard, input_map, output_map_small, prior, queries,
    scores,
    weights, work, strip, square, small, outer, inner, hidden, following, cotangent, previous, values, upstream, normed,
    activated, slopes, features, factors, gain_half, input_half, first_out, first_in,
    extra_out, extra_in, second_out, second_in, flats, everyone, rows_all, final,
    gather_send, gather_receive, own_weights, prior_done, entry_own, entry_send, entry_receive,
    forward_send, forward_receive, backward_send, backward_receive,
    first_send, first_receive, extra_send, extra_receive, second_send, second_receive,
    publish_send, publish_receive, final_send, final_receive,
):
    section, me = lax.axis_index("section"), lax.axis_index("dp")
    has_before, has_after = section > 0, section < sections - 1
    before, after = lax.max(section - 1, 0), lax.min(section + 1, sections - 1)
    side = lax.rem(lax.div(me, PAIR), 2)
    partner = flipped(me, PAIR)
    batches, example_length, width = inputs.shape
    entries, length = hidden.shape[0], hidden.shape[1]
    per_side = entries // 2
    cuts = per_side // batches
    half, value_width = weights.shape[1], weights.shape[2]
    rows = value_shard.shape[0]
    piece_rows = rows // PIECES
    stretch = PAIR * rows
    stretches = half // stretch
    size = work.shape[0]
    blocks = size // BLOCK
    feature_width = input_map.shape[0]
    signal_width = output_map_small.shape[0]
    chunks = forward_send.shape[1]
    chunk = half // chunks
    tiles = first_send.shape[1]
    tile = value_width // tiles
    group = 16
    shards = (value_shard, output_shard)
    value_map, output_map = weights.at[0], weights.at[1]
    events = gather_events(count)

    def gather_copy(number, array, piece, first):
        bit, mask = events[number]
        at = slot_of(mate(me, mask)) * PIECES + piece
        there = weights.at[array, span(at, piece_rows), :]
        here = shards[array].at[span(piece, piece_rows), :] if first else there
        return pltpu.make_async_remote_copy(
            src_ref=here,
            dst_ref=there,
            send_sem=gather_send.at[number, array, piece],
            recv_sem=gather_receive.at[number, array, piece],
            device_id={"dp": flipped(me, bit)},
            device_id_type=MESH,
        )

    def serve(array, piece):
        for number, (bit, mask) in enumerate(events):
            forwards = [later for later, (_, want) in enumerate(events) if want == bit | mask]
            if forwards:
                gather_copy(number, array, piece, False).wait_recv()
            for later in forwards:
                gather_copy(later, array, piece, False).start()

    def collect(array):
        for number, (bit, mask) in enumerate(events):
            if all(want != bit | mask for _, want in events):
                @pl.loop(0, PIECES)
                def _(piece):
                    gather_copy(number, array, piece, False).wait_recv()

        kept[array].wait()

    def entry_copy(kind, entry, part, remote):
        source = (inputs, targets)[kind]
        sink = (hidden, cotangent)[kind]
        wanted = 1 - side if remote else side
        lines = pl.ds((entry % cuts) * length, length)
        here = source.at[entry // cuts, lines, span(2 * part + wanted, stretch)]
        there = sink.at[side * per_side + entry, :, span(part, stretch)]
        if not remote:
            return pltpu.make_async_copy(here, there, entry_own.at[kind, entry, part])
        return pltpu.make_async_remote_copy(
            src_ref=here,
            dst_ref=there,
            send_sem=entry_send.at[kind, entry, part],
            recv_sem=entry_receive.at[kind, entry, part],
            device_id={"dp": partner},
            device_id_type=MESH,
        )

    def entry_wait(kind, batch):
        sink = (hidden, cotangent)[kind]
        owner, entry = lax.div(batch, per_side), lax.rem(batch, per_side)
        for part in range(stretches):
            there = sink.at[batch, :, span(part, stretch)]

            @pl.when(owner == side)
            def _():
                pltpu.make_async_copy(there, there, entry_own.at[kind, entry, part]).wait()

            @pl.when(owner != side)
            def _():
                pltpu.make_async_remote_copy(
                    src_ref=there,
                    dst_ref=there,
                    send_sem=entry_send.at[kind, entry, part],
                    recv_sem=entry_receive.at[kind, entry, part],
                    device_id={"dp": partner},
                    device_id_type=MESH,
                ).wait_recv()

    def hop(source, sink, send, receive, device, batch, piece):
        columns = span(piece, chunk)
        return pltpu.make_async_remote_copy(
            src_ref=source.at[batch, :, columns],
            dst_ref=sink.at[batch, :, columns],
            send_sem=send.at[batch, piece],
            recv_sem=receive.at[batch, piece],
            device_id={"section": device},
            device_id_type=MESH,
        )

    def forward_copy(batch, piece):
        return hop(following, hidden, forward_send, forward_receive, after, batch, piece)

    def backward_copy(batch, piece):
        return hop(previous, cotangent, backward_send, backward_receive, before, batch, piece)

    def swap(source, sink, send, receive, batch, at):
        columns = span(at, tile)
        return pltpu.make_async_remote_copy(
            src_ref=source.at[batch, :, columns],
            dst_ref=sink.at[batch, :, columns],
            send_sem=send.at[batch, at],
            recv_sem=receive.at[batch, at],
            device_id={"dp": partner},
            device_id_type=MESH,
        )

    def first_copy(batch, at):
        return swap(first_out, first_in, first_send, first_receive, batch, at)

    def second_copy(batch, at):
        return swap(second_out, second_in, second_send, second_receive, batch, at)

    def extra_copy(batch):
        return pltpu.make_async_remote_copy(
            src_ref=extra_out.at[batch],
            dst_ref=extra_in.at[batch],
            send_sem=extra_send.at[batch],
            recv_sem=extra_receive.at[batch],
            device_id={"dp": partner},
            device_id_type=MESH,
        )

    prior_copy = pltpu.make_async_copy(prior, work, prior_done)
    prior_copy.start()
    mine = span(slot_of(me), rows)
    kept = [
        pltpu.make_async_copy(shards[array], weights.at[array, mine, :], own_weights.at[array])
        for array in range(2)
    ]
    barrier = pltpu.get_barrier_semaphore()

    @pl.loop(1, count)
    def _(offset):
        pl.semaphore_signal(
            barrier, inc=1, device_id={"dp": lax.rem(me + offset, count)}, device_id_type=MESH
        )

    @pl.loop(1, sections)
    def _(offset):
        pl.semaphore_signal(
            barrier, inc=1, device_id={"section": lax.rem(section + offset, sections)},
            device_id_type=MESH,
        )

    pl.semaphore_wait(barrier, count + sections - 2)

    for kind, wanted in ((0, jnp.logical_not(has_before)), (1, jnp.logical_not(has_after))):
        @pl.when(wanted)
        def _():
            for entry in range(per_side):
                for part in range(stretches):
                    entry_copy(kind, entry, part, True).start()
                    entry_copy(kind, entry, part, False).start()

    for array in range(2):
        for piece in range(PIECES):
            for number, (_, mask) in enumerate(events):
                if mask == 0:
                    gather_copy(number, array, piece, True).start()
    for copy in kept:
        copy.start()

    input_half[...] = jnp.zeros_like(input_half)
    for part in range(stretches):
        there = pl.ds(part * stretch, stretch)
        here = span(2 * part + side, stretch)
        gain_half[:, there] = gain[:, here]
        input_half[:feature_width, there] = input_map[:, here]
    for target, shift in ((outer, True), (inner, False)):
        entry = lax.broadcasted_iota(jnp.int32, target.shape, 1)
        line = lax.broadcasted_iota(jnp.int32, target.shape, 0)
        place = lax.div(entry, feature_width) if shift else lax.rem(entry, feature_width)
        target[...] = jnp.where(place == line, 1.0, 0.0).astype(jnp.bfloat16)
    prior_copy.wait()

    @pl.loop(0, max(blocks, 2 * PIECES))
    def _(step):
        @pl.when(step < blocks)
        def _():
            sweep_strip(work, strip, square, step, BLOCK)
            sweep_rest(work, strip, step, BLOCK)

        @pl.when((step >= 4) & (step < 4 + 2 * PIECES // 2))
        def _():
            for extra in range(2):
                number = lax.min(lax.max((step - 4) * 2 + extra, 0), 2 * PIECES - 1)
                serve(lax.div(number, PIECES), lax.rem(number, PIECES))

    collect(0)

    def forward_first(batch):
        @pl.when(jnp.logical_not(has_before))
        def _():
            entry_wait(0, batch)

        total = jnp.zeros((length, 1), jnp.float32)
        for piece in range(chunks):
            columns = pl.ds(piece * chunk, chunk)

            @pl.when(has_before)
            def _():
                forward_copy(batch, piece).wait_recv()

            widened = hidden[batch, :, columns].astype(jnp.float32)
            total = total + jnp.sum(widened * widened, axis=-1, keepdims=True)
            normed[:, columns] = (widened * gain_half[:, columns]).astype(jnp.bfloat16)

        for at in range(tiles):
            columns = pl.ds(at * tile, tile)
            found = jnp.dot(
                normed[...], value_map[:, columns], preferred_element_type=jnp.float32
            )
            values[batch, :, columns] = found
            first_out[batch, :, columns] = found.astype(jnp.bfloat16)
            first_copy(batch, at).start()
            if at == 0:
                extras = lax.dot_general(
                    normed[...], input_half[...], CONTRACT_LAST,
                    preferred_element_type=jnp.float32,
                )
                lanes = lax.broadcasted_iota(jnp.int32, extras.shape, 1)
                extra_out[batch] = jnp.where(lanes == feature_width, total, extras)
                extra_copy(batch).start()

    def forward_second(batch):
        extra_copy(batch).wait_recv()
        both = extra_out[batch] + extra_in[batch]
        total = both[:, feature_width : feature_width + 1]
        factor = lax.rsqrt(total * (1.0 / width) + 1e-05)
        factors[batch] = factor
        features[batch] = (both[:, :feature_width] * factor).astype(jnp.bfloat16)

        for at in range(tiles):
            columns = pl.ds(at * tile, tile)
            first_copy(batch, at).wait_recv()
            partial = first_in[batch, :, columns].astype(jnp.float32)
            found = (values[batch, :, columns] + partial) * factor
            values[batch, :, columns] = found
            activated[:, columns] = (found / (1.0 + jnp.exp(-found))).astype(jnp.bfloat16)

        @pl.when(has_after)
        def _():
            for piece in range(chunks):
                columns = pl.ds(piece * chunk, chunk)
                branch = lax.dot_general(
                    activated[...], output_map[columns, :], CONTRACT_LAST,
                    preferred_element_type=jnp.float32,
                )
                following[batch, :, columns] = (
                    hidden[batch, :, columns].astype(jnp.float32) + branch
                ).astype(jnp.bfloat16)
                forward_copy(batch, piece).start()

    def backward_first(batch):
        for at in range(tiles):
            columns = pl.ds(at * tile, tile)
            found = jnp.dot(
                cotangent[batch], output_map[:, columns], preferred_element_type=jnp.float32
            )
            upstream[batch, :, columns] = found
            second_out[batch, :, columns] = found.astype(jnp.bfloat16)
            second_copy(batch, at).start()

    def backward_second(batch):
        total = jnp.zeros((length, 1), jnp.float32)
        for at in range(tiles):
            columns = pl.ds(at * tile, tile)
            second_copy(batch, at).wait_recv()
            arrived = upstream[batch, :, columns] + second_in[batch, :, columns].astype(jnp.float32)
            found = values[batch, :, columns]
            logistic = 1.0 / (1.0 + jnp.exp(-found))
            slope = (arrived * logistic * (1.0 + found * (1.0 - logistic))).astype(jnp.bfloat16)
            slopes[:, columns] = slope
            total = total + jnp.sum(slope.astype(jnp.float32) * found, axis=-1, keepdims=True)

        factor = factors[batch]
        shrink = total * (factor * factor) * (1.0 / width)

        @pl.when(has_before)
        def _():
            for piece in range(chunks):
                columns = pl.ds(piece * chunk, chunk)
                normed_grad = lax.dot_general(
                    slopes[...], value_map[columns, :], CONTRACT_LAST,
                    preferred_element_type=jnp.float32,
                )
                weighted = normed_grad * gain_half[:, columns]
                hidden_grad = (
                    factor * weighted - hidden[batch, :, columns].astype(jnp.float32) * shrink
                )
                previous[batch, :, columns] = (
                    cotangent[batch, :, columns].astype(jnp.float32) + hidden_grad
                ).astype(jnp.bfloat16)
                backward_copy(batch, piece).start()

        signals = lax.dot_general(
            slopes[...], output_map_small[...], CONTRACT_LAST, preferred_element_type=jnp.float32
        ).astype(jnp.bfloat16)
        left = jnp.dot(signals, outer[...], preferred_element_type=jnp.float32)
        right = jnp.dot(features[batch], inner[...], preferred_element_type=jnp.float32)
        flat = jnp.sum(left * right, axis=0, keepdims=True) * (1.0 / example_length)
        flats[lax.div(batch, per_side), pl.ds(lax.rem(batch, per_side), 1), :] = flat

    collect(1)

    @pl.when(jnp.logical_not(has_after))
    def _():
        @pl.loop(0, entries)
        def _(batch):
            entry_wait(1, batch)
            backward_first(batch)

    @pl.loop(0, entries + 1)
    def _(batch):
        @pl.when(batch < entries)
        def _():
            forward_first(lax.min(batch, entries - 1))

        @pl.when(batch > 0)
        def _():
            forward_second(lax.max(batch - 1, 0))

            @pl.when(jnp.logical_not(has_after))
            def _():
                backward_second(lax.max(batch - 1, 0))

    @pl.when(has_after)
    def _():
        @pl.loop(0, entries + 1)
        def _(batch):
            @pl.when(batch < entries)
            def _():
                for piece in range(chunks):
                    backward_copy(lax.min(batch, entries - 1), piece).wait_recv()

                backward_first(lax.min(batch, entries - 1))

            @pl.when(batch > 0)
            def _():
                backward_second(lax.max(batch - 1, 0))

    ours = flats[side]
    for entry in range(batches):
        gathered = ours[entry * cuts : entry * cuts + 1, :]
        for cut in range(1, cuts):
            gathered = gathered + ours[entry * cuts + cut : entry * cuts + cut + 1, :]
        everyone[me, entry : entry + 1, :] = gathered

    def publish(offset, origin):
        return pltpu.make_async_remote_copy(
            src_ref=everyone.at[origin],
            dst_ref=everyone.at[origin],
            send_sem=publish_send.at[offset],
            recv_sem=publish_receive.at[offset],
            device_id={"dp": lax.rem(me + offset, count)},
            device_id_type=MESH,
        )

    @pl.loop(1, count)
    def _(offset):
        publish(offset, me).start()

    @pl.loop(1, count)
    def _(offset):
        publish(offset, lax.rem(me + count - offset, count)).wait_recv()

    for device in range(count):
        rows_all[device * batches : (device + 1) * batches, :] = everyone[device]
    grads = rows_all[...]
    examples = count * batches
    product = jnp.dot(grads, work[...], precision=HIGHEST, preferred_element_type=jnp.float32)
    gram = -lax.dot_general(
        product, grads, CONTRACT_LAST, precision=HIGHEST, preferred_element_type=jnp.float32
    )
    shape = (examples, examples)
    diagonal = lax.broadcasted_iota(jnp.int32, shape, 0) == lax.broadcasted_iota(jnp.int32, shape, 1)
    small[...] = jnp.zeros_like(small)
    small[:, :examples] = gram + jnp.where(diagonal, 1.0, 0.0)
    sweep_square(small)
    inverse = -small[:, :examples]
    picked = lax.broadcasted_iota(jnp.int32, (8, examples), 0)
    columns = lax.broadcasted_iota(jnp.int32, (8, examples), 1)
    pick = jnp.where((columns == me * batches + picked) & (picked < batches), 1.0, 0.0)
    owners = lax.broadcasted_iota(jnp.int32, (examples, queries.shape[1]), 0)
    selector = jnp.where(owners == queries[...], 1.0, 0.0)
    picked_gram = jnp.dot(pick, gram, precision=HIGHEST, preferred_element_type=jnp.float32)
    chosen = jnp.dot(inverse, selector, precision=HIGHEST, preferred_element_type=jnp.float32)
    final[section] = jnp.dot(picked_gram, chosen, precision=HIGHEST, preferred_element_type=jnp.float32)

    def finish(offset, origin):
        return pltpu.make_async_remote_copy(
            src_ref=final.at[origin],
            dst_ref=final.at[origin],
            send_sem=final_send.at[offset],
            recv_sem=final_receive.at[offset],
            device_id={"section": lax.rem(section + offset, sections)},
            device_id_type=MESH,
        )

    @pl.loop(1, sections)
    def _(offset):
        finish(offset, section).start()

    @pl.loop(1, sections)
    def _(offset):
        finish(offset, lax.rem(section + sections - offset, sections)).wait_recv()

    result = final[0]
    for other in range(1, sections):
        result = result + final[other]
    scores[...] = result[: scores.shape[0], : scores.shape[1]]

    @pl.loop(1, sections)
    def _(offset):
        finish(offset, section).wait_send()

    @pl.loop(1, count)
    def _(offset):
        publish(offset, me).wait_send()

    for kind, wanted in ((0, jnp.logical_not(has_before)), (1, jnp.logical_not(has_after))):
        @pl.when(wanted)
        def _():
            for entry in range(per_side):
                for part in range(stretches):
                    entry_copy(kind, entry, part, True).wait_send()

    for number, (_, mask) in enumerate(events):
        for array in range(2):
            @pl.loop(0, PIECES)
            def _(piece):
                gather_copy(number, array, piece, mask == 0).wait_send()

    @pl.loop(0, entries)
    def _(batch):
        extra_copy(batch).wait_send()

        @pl.loop(0, tiles)
        def _(at):
            first_copy(batch, at).wait_send()
            second_copy(batch, at).wait_send()

        @pl.loop(0, chunks)
        def _(piece):
            @pl.when(has_after)
            def _():
                forward_copy(batch, piece).wait_send()

            @pl.when(has_before)
            def _():
                backward_copy(batch, piece).wait_send()


def window(
    inputs, targets, gain, value_shard, output_shard, input_map, output_map_small, prior, queries
):
    sections, count = lax.axis_size("section"), lax.axis_size("dp")
    batches, example_length, width = inputs.shape
    rows, value_width = value_shard.shape
    cuts = 1
    length = example_length // cuts
    entries = 2 * batches * cuts
    half = width // 2
    size = prior.shape[0]
    feature_width = input_map.shape[0]
    signal_width = output_map_small.shape[0]
    asked = queries.shape[0]
    padded = jnp.full((1, LANES * pl.cdiv(asked, LANES)), -1, jnp.int32)
    padded = lax.dynamic_update_slice(padded, queries[None, :], (0, 0))
    chunks, tiles = 4, 2
    events = len(gather_events(count))
    stretches = half // (PAIR * rows)
    dma = pltpu.SemaphoreType.DMA
    stream = pltpu.VMEM((entries, length, half), jnp.bfloat16)
    parts = pltpu.VMEM((entries, length, value_width), jnp.bfloat16)
    extra = pltpu.VMEM((entries, length, LANES), jnp.float32)
    anywhere = pl.BlockSpec(memory_space=pl.ANY)
    inside = pl.BlockSpec(memory_space=pltpu.VMEM)
    return pl.pallas_call(
        functools.partial(window_kernel, sections, count),
        out_shape=jax.ShapeDtypeStruct((batches, asked), jnp.float32),
        in_specs=[
            anywhere, anywhere, inside, anywhere, anywhere, inside, inside, anywhere, inside
        ],
        out_specs=inside,
        scratch_shapes=[
            pltpu.VMEM((2, half, value_width), jnp.bfloat16),
            pltpu.VMEM((size, size), jnp.float32),
            pltpu.VMEM((BLOCK, size), jnp.float32),
            pltpu.VMEM((BLOCK, BLOCK), jnp.float32),
            pltpu.VMEM((count * batches, LANES), jnp.float32),
            pltpu.VMEM((signal_width, size), jnp.bfloat16),
            pltpu.VMEM((feature_width, size), jnp.bfloat16),
            stream, stream, stream, stream,
            pltpu.VMEM((entries, length, value_width), jnp.float32),
            pltpu.VMEM((entries, length, value_width), jnp.float32),
            pltpu.VMEM((length, half), jnp.bfloat16),
            pltpu.VMEM((length, value_width), jnp.bfloat16),
            pltpu.VMEM((length, value_width), jnp.bfloat16),
            pltpu.VMEM((entries, length, feature_width), jnp.bfloat16),
            pltpu.VMEM((entries, length, 1), jnp.float32),
            pltpu.VMEM((1, half), jnp.float32),
            pltpu.VMEM((LANES, half), jnp.bfloat16),
            parts, parts, extra, extra, parts, parts,
            pltpu.VMEM((2, batches * cuts, size), jnp.float32),
            pltpu.VMEM((count, batches, size), jnp.float32),
            pltpu.VMEM((count * batches, size), jnp.float32),
            pltpu.VMEM((sections, 8, padded.shape[1]), jnp.float32),
            dma((events, 2, PIECES)), dma((events, 2, PIECES)), dma((2,)), dma,
            dma((2, batches * cuts, stretches)), dma((2, batches * cuts, stretches)),
            dma((2, batches * cuts, stretches)),
            dma((entries, chunks)), dma((entries, chunks)),
            dma((entries, chunks)), dma((entries, chunks)),
            dma((entries, tiles)), dma((entries, tiles)), dma((entries,)), dma((entries,)),
            dma((entries, tiles)), dma((entries, tiles)),
            dma((count,)), dma((count,)), dma((sections,)), dma((sections,)),
        ],
        compiler_params=pltpu.CompilerParams(
            collective_id=1, has_side_effects=True, vmem_limit_bytes=52 * 2**20
        ),
        name="window",
    )(
        inputs, targets, gain, value_shard, output_shard, input_map, output_map_small, prior,
        padded,
    )


def per_device(
    inputs,
    output_cotangent,
    lengths,
    query_examples,
    norm_gain,
    value_weight,
    output_weight,
    input_projection,
    output_projection,
    fisher_prior,
):
    batches = lengths.shape[0]
    example_rows = inputs.shape[0] // batches
    width = inputs.shape[1]
    positions = jnp.arange(example_rows, dtype=jnp.int32)
    keep = (positions[None, :] < lengths[:, None]).astype(jnp.bfloat16)
    targets = output_cotangent.reshape(batches, example_rows, width) * keep[:, :, None]
    return window(
        inputs.reshape(batches, example_rows, width), targets, norm_gain.astype(jnp.float32),
        value_weight[0], output_weight[0], input_projection[0], output_projection[0],
        fisher_prior[0], query_examples,
    )


def solution(mesh):
    placed = (
        P("dp", None),
        P("dp", None),
        P("dp"),
        P(),
        P("section", None),
        P("section", "dp", None),
        P("section", "dp", None),
        P("section", None, None),
        P("section", None, None),
        P("section", None, None),
    )
    return jax.shard_map(
        per_device, mesh=mesh, in_specs=placed, out_specs=P("dp", None), check_vma=False
    )
```

```python
import functools

import jax
import jax.numpy as jnp
from jax import lax
from jax.experimental import pallas as pl
from jax.experimental.pallas import tpu as pltpu
from jax.sharding import PartitionSpec as P


HIGHEST = lax.Precision.HIGHEST


GROUP = 8


def small_inverse(held):
    count = len(held)
    held = [list(line) for line in held]
    for pivot in range(count):
        scale = 1.0 / held[pivot][pivot]
        line = list(held[pivot])
        scaled = [value * scale for value in line]
        for i in range(count):
            for j in range(i, count):
                if i != pivot and j != pivot:
                    held[i][j] = held[j][i] = held[i][j] - line[i] * scaled[j]
        for j in range(count):
            held[pivot][j] = held[j][pivot] = scaled[j]
        held[pivot][pivot] = -scale
    return [[-value for value in line] for line in held]


def sweep_square(square):
    rows, columns = square.shape
    lanes = lax.broadcasted_iota(jnp.int32, (GROUP, columns), 1)
    lines = lax.broadcasted_iota(jnp.int32, (GROUP, columns), 0)
    wide = lax.broadcasted_iota(jnp.int32, (rows, columns), 1)

    @pl.loop(0, rows // GROUP)
    def _(at):
        base = at * GROUP
        part = pl.ds(pl.multiple_of(base, GROUP), GROUP)
        panel = square[part, :]
        corner = [
            jnp.sum(jnp.where(lanes == base + k, panel, 0.0), axis=1, keepdims=True)
            for k in range(GROUP)
        ]
        spread = [
            [jnp.broadcast_to(corner[k][i : i + 1, :], (1, columns)) for k in range(GROUP)]
            for i in range(GROUP)
        ]
        inverse = small_inverse(spread)
        inside = (lanes >= base) & (lanes < base + GROUP)
        unit = jnp.where(lanes - base == lines, 1.0, 0.0)
        source = jnp.where(inside, unit, panel)
        built = []
        for i in range(GROUP):
            total = inverse[i][0] * source[:1, :]
            for k in range(1, GROUP):
                total = total + inverse[i][k] * source[k : k + 1, :]
            built.append(total)
        strip = jnp.concatenate(built, axis=0)
        signed = jnp.where(inside, -strip, strip)
        full = square[...]
        within = (wide >= base) & (wide < base + GROUP)
        updated = jnp.where(within, 0.0, full)
        for k in range(GROUP):
            column = jnp.sum(jnp.where(wide == base + k, full, 0.0), axis=1, keepdims=True)
            updated = updated - column * signed[k : k + 1, :]
        square[...] = updated
        square[part, :] = signed


def sweep_strip(work, strip, square, step, block):
    part = pl.ds(pl.multiple_of(step * block, block), block)
    square[...] = work[part, part]
    sweep_square(square)
    corner = square[...]
    strip[...] = -jnp.dot(
        corner, work[part, :], precision=HIGHEST, preferred_element_type=jnp.float32
    )
    strip[:, part] = corner


def sweep_rest(work, strip, step, block):
    span = pl.ds(pl.multiple_of(step * block, block), block)

    @pl.loop(0, work.shape[0] // block)
    def _(other):
        across = pl.ds(pl.multiple_of(other * block, block), block)

        @pl.when(other != step)
        def _():
            work[across, :] -= jnp.dot(
                work[span, across].T, strip[...], precision=HIGHEST,
                preferred_element_type=jnp.float32,
            )
            work[across, span] = strip[:, across].T

    work[span, :] = strip[...]


MESH = pl.DeviceIdType.MESH
CONTRACT_LAST = (((1,), (1,)), ((), ()))
PAIR = 2
PIECES = 4
LAG = 4
LEAD = 3
RATE = 2
BLOCK = 128
LANES = 128


def flipped(device, bit):
    return device + (1 - 2 * lax.rem(lax.div(device, bit), 2)) * bit


def mate(device, mask):
    bit = 1
    while bit <= mask:
        if mask & bit:
            device = flipped(device, bit)
        bit *= 2
    return device


def slot_of(device):
    return lax.div(device, 2 * PAIR) * PAIR + lax.rem(device, PAIR)


def gather_events(count):
    bits = []
    bit = count // 2
    while bit >= 1:
        if bit != PAIR:
            bits.append(bit)
        bit //= 2
    held, events = [0], []
    for bit in bits:
        events += [(bit, mask) for mask in held]
        held += [mask | bit for mask in held]
    return events


def span(index, size):
    return pl.ds(pl.multiple_of(index * size, size), size)


def window_kernel(
    sections, count,
    inputs, targets, gain, lengths, value_shard, output_shard, input_map, output_map_small, prior,
    queries, scores,
    weights, work, strip, square, small, outer, inner, hidden, following, cotangent, previous, values, upstream, normed,
    activated, slopes, features, factors, gain_half, input_half, first_out, first_in,
    extra_own, extra_out, extra_in, staging, second_out, second_in, flats, everyone, rows_all, final,
    gather_send, gather_receive, own_weights, prior_done, staged, entry_own, entry_send, entry_receive,
    forward_send, forward_receive, backward_send, backward_receive,
    first_send, first_receive, extra_send, extra_receive, second_send, second_receive,
    publish_send, publish_receive, final_send, final_receive, turn,
):
    section, me = lax.axis_index("section"), lax.axis_index("dp")
    has_before, has_after = section > 0, section < sections - 1
    before, after = lax.max(section - 1, 0), lax.min(section + 1, sections - 1)
    side = lax.rem(lax.div(me, PAIR), 2)
    follows = lax.rem(section, 2) == 1
    leads = jnp.logical_not(follows)
    twin = section + 1 - 2 * lax.rem(section, 2)
    partner = flipped(me, PAIR)
    batches, example_length, width = inputs.shape
    entries, length = hidden.shape[0], hidden.shape[1]
    per_side = entries // 2
    cuts = per_side // batches
    half, value_width = weights.shape[1], weights.shape[2]
    rows = value_shard.shape[0]
    piece_rows = rows // PIECES
    stretch = PAIR * rows
    stretches = half // stretch
    size = work.shape[0]
    blocks = size // BLOCK
    feature_width = input_map.shape[0]
    signal_width = output_map_small.shape[0]
    chunks = forward_send.shape[1]
    chunk = half // chunks
    tiles = first_send.shape[1]
    tile = value_width // tiles
    group = 16
    shards = (value_shard, output_shard)
    value_map, output_map = weights.at[0], weights.at[1]
    events = gather_events(count)

    def gather_copy(number, array, piece, first):
        bit, mask = events[number]
        at = slot_of(mate(me, mask)) * PIECES + piece
        there = weights.at[array, span(at, piece_rows), :]
        here = shards[array].at[span(piece, piece_rows), :] if first else there
        return pltpu.make_async_remote_copy(
            src_ref=here,
            dst_ref=there,
            send_sem=gather_send.at[number, array, piece],
            recv_sem=gather_receive.at[number, array, piece],
            device_id={"dp": flipped(me, bit)},
            device_id_type=MESH,
        )

    def start_gather():
        for array in range(2):
            for piece in range(PIECES):
                for number, (_, mask) in enumerate(events):
                    if mask == 0:
                        gather_copy(number, array, piece, True).start()

    def serve(array, piece):
        for number, (bit, mask) in enumerate(events):
            forwards = [later for later, (_, want) in enumerate(events) if want == bit | mask]
            if forwards:
                gather_copy(number, array, piece, False).wait_recv()
            for later in forwards:
                gather_copy(later, array, piece, False).start()

    def collect(array):
        for number, (bit, mask) in enumerate(events):
            if all(want != bit | mask for _, want in events):
                @pl.loop(0, PIECES)
                def _(piece):
                    gather_copy(number, array, piece, False).wait_recv()

        kept[array].wait()

    def entry_copy(kind, entry, part, remote):
        source = (inputs, staging)[kind]
        sink = (hidden, cotangent)[kind]
        wanted = 1 - side if remote else side
        lines = pl.ds((entry % cuts) * length, length)
        here = source.at[entry // cuts, lines, span(2 * part + wanted, stretch)]
        there = sink.at[side * per_side + entry, :, span(part, stretch)]
        if not remote:
            return pltpu.make_async_copy(here, there, entry_own.at[kind, entry, part])
        return pltpu.make_async_remote_copy(
            src_ref=here,
            dst_ref=there,
            send_sem=entry_send.at[kind, entry, part],
            recv_sem=entry_receive.at[kind, entry, part],
            device_id={"dp": partner},
            device_id_type=MESH,
        )

    def entry_wait(kind, batch):
        sink = (hidden, cotangent)[kind]
        owner, entry = lax.div(batch, per_side), lax.rem(batch, per_side)
        for part in range(stretches):
            there = sink.at[batch, :, span(part, stretch)]

            @pl.when(owner == side)
            def _():
                pltpu.make_async_copy(there, there, entry_own.at[kind, entry, part]).wait()

            @pl.when(owner != side)
            def _():
                pltpu.make_async_remote_copy(
                    src_ref=there,
                    dst_ref=there,
                    send_sem=entry_send.at[kind, entry, part],
                    recv_sem=entry_receive.at[kind, entry, part],
                    device_id={"dp": partner},
                    device_id_type=MESH,
                ).wait_recv()

    def hop(source, sink, send, receive, device, batch, piece):
        columns = span(piece, chunk)
        return pltpu.make_async_remote_copy(
            src_ref=source.at[batch, :, columns],
            dst_ref=sink.at[batch, :, columns],
            send_sem=send.at[batch, piece],
            recv_sem=receive.at[batch, piece],
            device_id={"section": device},
            device_id_type=MESH,
        )

    def forward_copy(batch, piece):
        return hop(following, hidden, forward_send, forward_receive, after, batch, piece)

    def backward_copy(batch, piece):
        return hop(previous, cotangent, backward_send, backward_receive, before, batch, piece)

    def swap(source, sink, send, receive, batch, at):
        columns = span(at, tile)
        return pltpu.make_async_remote_copy(
            src_ref=source.at[batch, :, columns],
            dst_ref=sink.at[batch, :, columns],
            send_sem=send.at[batch, at],
            recv_sem=receive.at[batch, at],
            device_id={"dp": partner},
            device_id_type=MESH,
        )

    def first_copy(batch, at):
        return swap(first_out, first_in, first_send, first_receive, batch, at)

    def second_copy(batch, at):
        return swap(second_out, second_in, second_send, second_receive, batch, at)

    def extra_copy(batch):
        return pltpu.make_async_remote_copy(
            src_ref=extra_out.at[batch],
            dst_ref=extra_in.at[batch],
            send_sem=extra_send.at[batch],
            recv_sem=extra_receive.at[batch],
            device_id={"dp": partner},
            device_id_type=MESH,
        )

    prior_copy = pltpu.make_async_copy(prior, work, prior_done)
    prior_copy.start()
    stage_copy = pltpu.make_async_copy(targets, staging, staged)

    @pl.when(jnp.logical_not(has_after))
    def _():
        stage_copy.start()

    mine = span(slot_of(me), rows)
    kept = [
        pltpu.make_async_copy(shards[array], weights.at[array, mine, :], own_weights.at[array])
        for array in range(2)
    ]
    barrier = pltpu.get_barrier_semaphore()

    @pl.loop(1, count)
    def _(offset):
        pl.semaphore_signal(
            barrier, inc=1, device_id={"dp": lax.rem(me + offset, count)}, device_id_type=MESH
        )

    @pl.loop(1, sections)
    def _(offset):
        pl.semaphore_signal(
            barrier, inc=1, device_id={"section": lax.rem(section + offset, sections)},
            device_id_type=MESH,
        )

    pl.semaphore_wait(barrier, count + sections - 2)

    @pl.when(leads)
    def _():
        start_gather()

    def start_entries(kind):
        for entry in range(per_side):
            for part in range(stretches):
                entry_copy(kind, entry, part, True).start()
                entry_copy(kind, entry, part, False).start()

    @pl.when(jnp.logical_not(has_before))
    def _():
        start_entries(0)

    @pl.when(jnp.logical_not(has_after))
    def _():
        stage_copy.wait()
        line = lax.broadcasted_iota(jnp.int32, (example_length, 1), 0)
        for entry in range(batches):
            live = jnp.where(line < lengths[:, entry : entry + 1], 1.0, 0.0)
            staging[entry] = staging[entry] * live.astype(jnp.bfloat16)

        start_entries(1)

    for copy in kept:
        copy.start()

    input_half[...] = jnp.zeros_like(input_half)
    for part in range(stretches):
        there = pl.ds(part * stretch, stretch)
        here = span(2 * part + side, stretch)
        gain_half[:, there] = gain[:, here].astype(jnp.float32)
        input_half[:feature_width, there] = input_map[:, here]
    for target, shift in ((outer, True), (inner, False)):
        entry = lax.broadcasted_iota(jnp.int32, target.shape, 1)
        line = lax.broadcasted_iota(jnp.int32, target.shape, 0)
        place = lax.div(entry, feature_width) if shift else lax.rem(entry, feature_width)
        target[...] = jnp.where(place == line, 1.0, 0.0).astype(jnp.bfloat16)
    prior_copy.wait()

    def sweep(step):
        sweep_strip(work, strip, square, step, BLOCK)
        sweep_rest(work, strip, step, BLOCK)

    late = lax.rem(section, 2) * LAG
    served = pl.cdiv(LEAD + pl.cdiv(2 * PIECES, RATE), 2)
    stop = lax.min(late + served, blocks)

    def serve_at(point):
        for extra in range(RATE):
            number = point * RATE + extra

            @pl.when((number >= 0) & (number < 2 * PIECES))
            def _():
                bounded = lax.min(lax.max(number, 0), 2 * PIECES - 1)
                serve(lax.div(bounded, PIECES), lax.rem(bounded, PIECES))

    @pl.loop(0, late + served)
    def _(step):
        @pl.when(follows & (step == LAG))
        def _():
            pl.semaphore_wait(turn, 1)
            start_gather()

        point = 2 * (step - late) - LEAD

        @pl.when(step < blocks)
        def _():
            sweep_strip(work, strip, square, step, BLOCK)

        serve_at(point)

        @pl.when(step < blocks)
        def _():
            sweep_rest(work, strip, step, BLOCK)

        serve_at(point + 1)

    collect(0)
    collect(1)

    @pl.when(leads)
    def _():
        pl.semaphore_signal(turn, inc=1, device_id={"section": twin}, device_id_type=MESH)

    first_stop = lax.select(has_before, blocks, stop)

    @pl.loop(stop, first_stop)
    def _(step):
        sweep(step)

    def forward_first(batch):
        @pl.when(jnp.logical_not(has_before))
        def _():
            entry_wait(0, batch)

        total = jnp.zeros((length, 1), jnp.float32)
        for piece in range(chunks):
            columns = pl.ds(piece * chunk, chunk)

            @pl.when(has_before)
            def _():
                forward_copy(batch, piece).wait_recv()

            widened = hidden[batch, :, columns].astype(jnp.float32)
            total = total + jnp.sum(widened * widened, axis=-1, keepdims=True)
            normed[:, columns] = (widened * gain_half[:, columns]).astype(jnp.bfloat16)

        for at in range(tiles):
            columns = pl.ds(at * tile, tile)
            found = jnp.dot(
                normed[...], value_map[:, columns], preferred_element_type=jnp.float32
            )
            values[batch, :, columns] = found
            first_out[batch, :, columns] = found.astype(jnp.bfloat16)
            first_copy(batch, at).start()
            if at == 0:
                extras = lax.dot_general(
                    normed[...], input_half[...], CONTRACT_LAST,
                    preferred_element_type=jnp.float32,
                )
                lanes = lax.broadcasted_iota(jnp.int32, extras.shape, 1)
                extra_own[batch] = jnp.where(lanes == feature_width, total, extras)
                high = total.astype(jnp.bfloat16).astype(jnp.float32)
                extras = jnp.where(lanes == feature_width, high, extras)
                extras = jnp.where(lanes == feature_width + 1, total - high, extras)
                extra_out[batch] = extras.astype(jnp.bfloat16)
                extra_copy(batch).start()

    def forward_second(batch):
        extra_copy(batch).wait_recv()
        arrived = extra_in[batch].astype(jnp.float32)
        both = extra_own[batch] + arrived
        total = (
            both[:, feature_width : feature_width + 1]
            + arrived[:, feature_width + 1 : feature_width + 2]
        )
        factor = lax.rsqrt(total * (1.0 / width) + 1e-05)
        factors[batch] = factor
        features[batch] = (both[:, :feature_width] * factor).astype(jnp.bfloat16)

        for at in range(tiles):
            columns = pl.ds(at * tile, tile)
            first_copy(batch, at).wait_recv()
            partial = first_in[batch, :, columns].astype(jnp.float32)
            found = (values[batch, :, columns] + partial) * factor
            values[batch, :, columns] = found
            activated[:, columns] = (found / (1.0 + jnp.exp(-found))).astype(jnp.bfloat16)

        @pl.when(has_after)
        def _():
            for piece in range(chunks):
                columns = pl.ds(piece * chunk, chunk)
                branch = lax.dot_general(
                    activated[...], output_map[columns, :], CONTRACT_LAST,
                    preferred_element_type=jnp.float32,
                )
                following[batch, :, columns] = (
                    hidden[batch, :, columns].astype(jnp.float32) + branch
                ).astype(jnp.bfloat16)
                forward_copy(batch, piece).start()

    def backward_first(batch):
        for at in range(tiles):
            columns = pl.ds(at * tile, tile)
            found = jnp.dot(
                cotangent[batch], output_map[:, columns], preferred_element_type=jnp.float32
            )
            upstream[batch, :, columns] = found
            second_out[batch, :, columns] = found.astype(jnp.bfloat16)
            second_copy(batch, at).start()

    def backward_second(batch):
        total = jnp.zeros((length, 1), jnp.float32)
        for at in range(tiles):
            columns = pl.ds(at * tile, tile)
            second_copy(batch, at).wait_recv()
            arrived = upstream[batch, :, columns] + second_in[batch, :, columns].astype(jnp.float32)
            found = values[batch, :, columns]
            logistic = 1.0 / (1.0 + jnp.exp(-found))
            slope = (arrived * logistic * (1.0 + found * (1.0 - logistic))).astype(jnp.bfloat16)
            slopes[:, columns] = slope
            total = total + jnp.sum(slope.astype(jnp.float32) * found, axis=-1, keepdims=True)

        factor = factors[batch]
        shrink = total * (factor * factor) * (1.0 / width)

        @pl.when(has_before)
        def _():
            for piece in range(chunks):
                columns = pl.ds(piece * chunk, chunk)
                normed_grad = lax.dot_general(
                    slopes[...], value_map[columns, :], CONTRACT_LAST,
                    preferred_element_type=jnp.float32,
                )
                weighted = normed_grad * gain_half[:, columns]
                hidden_grad = (
                    factor * weighted - hidden[batch, :, columns].astype(jnp.float32) * shrink
                )
                previous[batch, :, columns] = (
                    cotangent[batch, :, columns].astype(jnp.float32) + hidden_grad
                ).astype(jnp.bfloat16)
                backward_copy(batch, piece).start()

        signals = lax.dot_general(
            slopes[...], output_map_small[...], CONTRACT_LAST, preferred_element_type=jnp.float32
        ).astype(jnp.bfloat16)
        left = jnp.dot(signals, outer[...], preferred_element_type=jnp.float32)
        right = jnp.dot(features[batch], inner[...], preferred_element_type=jnp.float32)
        flat = jnp.sum(left * right, axis=0, keepdims=True) * (1.0 / example_length)
        flats[lax.div(batch, per_side), pl.ds(lax.rem(batch, per_side), 1), :] = flat

    @pl.when(jnp.logical_not(has_after))
    def _():
        @pl.loop(0, entries)
        def _(batch):
            entry_wait(1, batch)
            backward_first(batch)

    @pl.loop(0, entries + 1)
    def _(batch):
        @pl.when(batch < entries)
        def _():
            forward_first(lax.min(batch, entries - 1))

        @pl.when(batch > 0)
        def _():
            forward_second(lax.max(batch - 1, 0))

            @pl.when(jnp.logical_not(has_after))
            def _():
                backward_second(lax.max(batch - 1, 0))

    @pl.loop(first_stop, blocks)
    def _(step):
        sweep(step)

    @pl.when(has_after)
    def _():
        @pl.loop(0, entries + 1)
        def _(batch):
            @pl.when(batch < entries)
            def _():
                for piece in range(chunks):
                    backward_copy(lax.min(batch, entries - 1), piece).wait_recv()

                backward_first(lax.min(batch, entries - 1))

            @pl.when(batch > 0)
            def _():
                backward_second(lax.max(batch - 1, 0))

    ours = flats[side]
    for entry in range(batches):
        gathered = ours[entry * cuts : entry * cuts + 1, :]
        for cut in range(1, cuts):
            gathered = gathered + ours[entry * cuts + cut : entry * cuts + cut + 1, :]
        everyone[me, entry : entry + 1, :] = gathered

    def publish(offset, origin):
        return pltpu.make_async_remote_copy(
            src_ref=everyone.at[origin],
            dst_ref=everyone.at[origin],
            send_sem=publish_send.at[offset],
            recv_sem=publish_receive.at[offset],
            device_id={"dp": lax.rem(me + offset, count)},
            device_id_type=MESH,
        )

    @pl.loop(1, count)
    def _(offset):
        publish(offset, me).start()

    @pl.loop(1, count)
    def _(offset):
        publish(offset, lax.rem(me + count - offset, count)).wait_recv()

    for device in range(count):
        rows_all[device * batches : (device + 1) * batches, :] = everyone[device]
    grads = rows_all[...]
    examples = count * batches
    product = jnp.dot(grads, work[...], precision=HIGHEST, preferred_element_type=jnp.float32)
    gram = -lax.dot_general(
        product, grads, CONTRACT_LAST, precision=HIGHEST, preferred_element_type=jnp.float32
    )
    shape = (examples, examples)
    diagonal = lax.broadcasted_iota(jnp.int32, shape, 0) == lax.broadcasted_iota(jnp.int32, shape, 1)
    small[...] = jnp.zeros_like(small)
    small[:, :examples] = gram + jnp.where(diagonal, 1.0, 0.0)
    sweep_square(small)
    inverse = -small[:, :examples]
    picked = lax.broadcasted_iota(jnp.int32, (8, examples), 0)
    columns = lax.broadcasted_iota(jnp.int32, (8, examples), 1)
    pick = jnp.where((columns == me * batches + picked) & (picked < batches), 1.0, 0.0)
    owners = lax.broadcasted_iota(jnp.int32, (examples, queries.shape[1]), 0)
    selector = jnp.where(owners == queries[...], 1.0, 0.0)
    picked_gram = jnp.dot(pick, gram, precision=HIGHEST, preferred_element_type=jnp.float32)
    chosen = jnp.dot(inverse, selector, precision=HIGHEST, preferred_element_type=jnp.float32)
    final[section] = jnp.dot(picked_gram, chosen, precision=HIGHEST, preferred_element_type=jnp.float32)

    def finish(offset, origin):
        return pltpu.make_async_remote_copy(
            src_ref=final.at[origin],
            dst_ref=final.at[origin],
            send_sem=final_send.at[offset],
            recv_sem=final_receive.at[offset],
            device_id={"section": lax.rem(section + offset, sections)},
            device_id_type=MESH,
        )

    @pl.loop(1, sections)
    def _(offset):
        finish(offset, section).start()

    @pl.loop(1, sections)
    def _(offset):
        finish(offset, lax.rem(section + sections - offset, sections)).wait_recv()

    result = final[0]
    for other in range(1, sections):
        result = result + final[other]
    scores[...] = result[: scores.shape[0], : scores.shape[1]]

    @pl.loop(1, sections)
    def _(offset):
        finish(offset, section).wait_send()

    @pl.loop(1, count)
    def _(offset):
        publish(offset, me).wait_send()

    for kind, wanted in ((0, jnp.logical_not(has_before)), (1, jnp.logical_not(has_after))):
        @pl.when(wanted)
        def _():
            for entry in range(per_side):
                for part in range(stretches):
                    entry_copy(kind, entry, part, True).wait_send()

    for number, (_, mask) in enumerate(events):
        for array in range(2):
            @pl.loop(0, PIECES)
            def _(piece):
                gather_copy(number, array, piece, mask == 0).wait_send()

    @pl.loop(0, entries)
    def _(batch):
        extra_copy(batch).wait_send()

        @pl.loop(0, tiles)
        def _(at):
            first_copy(batch, at).wait_send()
            second_copy(batch, at).wait_send()

        @pl.loop(0, chunks)
        def _(piece):
            @pl.when(has_after)
            def _():
                forward_copy(batch, piece).wait_send()

            @pl.when(has_before)
            def _():
                backward_copy(batch, piece).wait_send()


def window(
    inputs, targets, gain, lengths, value_shard, output_shard, input_map, output_map_small, prior, queries
):
    sections, count = lax.axis_size("section"), lax.axis_size("dp")
    batches, example_length, width = inputs.shape
    rows, value_width = value_shard.shape
    cuts = 1
    length = example_length // cuts
    entries = 2 * batches * cuts
    half = width // 2
    size = prior.shape[0]
    feature_width = input_map.shape[0]
    signal_width = output_map_small.shape[0]
    asked = queries.shape[0]
    chunks, tiles = 4, 2
    events = len(gather_events(count))
    stretches = half // (PAIR * rows)
    dma = pltpu.SemaphoreType.DMA
    stream = pltpu.VMEM((entries, length, half), jnp.bfloat16)
    parts = pltpu.VMEM((entries, length, value_width), jnp.bfloat16)
    extra = pltpu.VMEM((entries, length, LANES), jnp.bfloat16)
    anywhere = pl.BlockSpec(memory_space=pl.ANY)
    inside = pl.BlockSpec(memory_space=pltpu.VMEM)
    return pl.pallas_call(
        functools.partial(window_kernel, sections, count),
        out_shape=jax.ShapeDtypeStruct((batches, asked), jnp.float32),
        in_specs=[
            anywhere, anywhere, inside, inside, anywhere, anywhere, inside, inside, anywhere,
            inside,
        ],
        out_specs=inside,
        scratch_shapes=[
            pltpu.VMEM((2, half, value_width), jnp.bfloat16),
            pltpu.VMEM((size, size), jnp.float32),
            pltpu.VMEM((BLOCK, size), jnp.float32),
            pltpu.VMEM((BLOCK, BLOCK), jnp.float32),
            pltpu.VMEM((count * batches, LANES), jnp.float32),
            pltpu.VMEM((signal_width, size), jnp.bfloat16),
            pltpu.VMEM((feature_width, size), jnp.bfloat16),
            stream, stream, stream, stream,
            pltpu.VMEM((entries, length, value_width), jnp.float32),
            pltpu.VMEM((entries, length, value_width), jnp.float32),
            pltpu.VMEM((length, half), jnp.bfloat16),
            pltpu.VMEM((length, value_width), jnp.bfloat16),
            pltpu.VMEM((length, value_width), jnp.bfloat16),
            pltpu.VMEM((entries, length, feature_width), jnp.bfloat16),
            pltpu.VMEM((entries, length, 1), jnp.float32),
            pltpu.VMEM((1, half), jnp.float32),
            pltpu.VMEM((LANES, half), jnp.bfloat16),
            parts, parts, pltpu.VMEM((entries, length, LANES), jnp.float32), extra, extra,
            pltpu.VMEM((batches, example_length, width), jnp.bfloat16), parts, parts,
            pltpu.VMEM((2, batches * cuts, size), jnp.float32),
            pltpu.VMEM((count, batches, size), jnp.float32),
            pltpu.VMEM((count * batches, size), jnp.float32),
            pltpu.VMEM((sections, 8, asked), jnp.float32),
            dma((events, 2, PIECES)), dma((events, 2, PIECES)), dma((2,)), dma, dma,
            dma((2, batches * cuts, stretches)), dma((2, batches * cuts, stretches)),
            dma((2, batches * cuts, stretches)),
            dma((entries, chunks)), dma((entries, chunks)),
            dma((entries, chunks)), dma((entries, chunks)),
            dma((entries, tiles)), dma((entries, tiles)), dma((entries,)), dma((entries,)),
            dma((entries, tiles)), dma((entries, tiles)),
            dma((count,)), dma((count,)), dma((sections,)), dma((sections,)),
            pltpu.SemaphoreType.REGULAR,
        ],
        compiler_params=pltpu.CompilerParams(
            collective_id=1, has_side_effects=True, vmem_limit_bytes=52 * 2**20
        ),
        name="window",
    )(
        inputs, targets, gain, lengths, value_shard, output_shard, input_map, output_map_small,
        prior, queries[None, :],
    )


def per_device(
    inputs,
    output_cotangent,
    lengths,
    query_examples,
    norm_gain,
    value_weight,
    output_weight,
    input_projection,
    output_projection,
    fisher_prior,
):
    batches = lengths.shape[0]
    example_rows = inputs.shape[0] // batches
    width = inputs.shape[1]
    targets = output_cotangent.reshape(batches, example_rows, width)
    return window(
        inputs.reshape(batches, example_rows, width), targets, norm_gain, lengths[None, :],
        value_weight[0], output_weight[0], input_projection[0], output_projection[0],
        fisher_prior[0], query_examples,
    )


def solution(mesh):
    placed = (
        P("dp", None),
        P("dp", None),
        P("dp"),
        P(),
        P("section", None),
        P("section", "dp", None),
        P("section", "dp", None),
        P("section", None, None),
        P("section", None, None),
        P("section", None, None),
    )
    return jax.shard_map(
        per_device, mesh=mesh, in_specs=placed, out_specs=P("dp", None), check_vma=False
    )
```

```python
import functools

import jax
import jax.numpy as jnp
from jax import lax
from jax.experimental import pallas as pl
from jax.experimental.pallas import tpu as pltpu
from jax.sharding import PartitionSpec as P


HIGHEST = lax.Precision.HIGHEST


GROUP = 8


def small_inverse(held):
    count = len(held)
    held = [list(line) for line in held]
    for pivot in range(count):
        scale = 1.0 / held[pivot][pivot]
        line = list(held[pivot])
        scaled = [value * scale for value in line]
        for i in range(count):
            for j in range(i, count):
                if i != pivot and j != pivot:
                    held[i][j] = held[j][i] = held[i][j] - line[i] * scaled[j]
        for j in range(count):
            held[pivot][j] = held[j][pivot] = scaled[j]
        held[pivot][pivot] = -scale
    return [[-value for value in line] for line in held]


def sweep_square(square):
    rows, columns = square.shape
    lanes = lax.broadcasted_iota(jnp.int32, (GROUP, columns), 1)
    lines = lax.broadcasted_iota(jnp.int32, (GROUP, columns), 0)
    wide = lax.broadcasted_iota(jnp.int32, (rows, columns), 1)

    @pl.loop(0, rows // GROUP)
    def _(at):
        base = at * GROUP
        part = pl.ds(pl.multiple_of(base, GROUP), GROUP)
        panel = square[part, :]
        corner = [
            jnp.sum(jnp.where(lanes == base + k, panel, 0.0), axis=1, keepdims=True)
            for k in range(GROUP)
        ]
        spread = [
            [jnp.broadcast_to(corner[k][i : i + 1, :], (1, columns)) for k in range(GROUP)]
            for i in range(GROUP)
        ]
        inverse = small_inverse(spread)
        inside = (lanes >= base) & (lanes < base + GROUP)
        unit = jnp.where(lanes - base == lines, 1.0, 0.0)
        source = jnp.where(inside, unit, panel)
        built = []
        for i in range(GROUP):
            total = inverse[i][0] * source[:1, :]
            for k in range(1, GROUP):
                total = total + inverse[i][k] * source[k : k + 1, :]
            built.append(total)
        strip = jnp.concatenate(built, axis=0)
        signed = jnp.where(inside, -strip, strip)
        full = square[...]
        within = (wide >= base) & (wide < base + GROUP)
        updated = jnp.where(within, 0.0, full)
        for k in range(GROUP):
            column = jnp.sum(jnp.where(wide == base + k, full, 0.0), axis=1, keepdims=True)
            updated = updated - column * signed[k : k + 1, :]
        square[...] = updated
        square[part, :] = signed


def sweep_strip(work, strip, square, step, block):
    part = pl.ds(pl.multiple_of(step * block, block), block)
    square[...] = work[part, part]
    sweep_square(square)
    corner = square[...]
    strip[...] = -jnp.dot(
        corner, work[part, :], precision=HIGHEST, preferred_element_type=jnp.float32
    )
    strip[:, part] = corner


def sweep_rest(work, strip, step, block):
    span = pl.ds(pl.multiple_of(step * block, block), block)

    @pl.loop(0, work.shape[0] // block)
    def _(other):
        across = pl.ds(pl.multiple_of(other * block, block), block)

        @pl.when(other != step)
        def _():
            work[across, :] -= jnp.dot(
                work[span, across].T, strip[...], precision=HIGHEST,
                preferred_element_type=jnp.float32,
            )
            work[across, span] = strip[:, across].T

    work[span, :] = strip[...]


MESH = pl.DeviceIdType.MESH
CONTRACT_LAST = (((1,), (1,)), ((), ()))
PAIR = 2
PIECES = 4
EAGER = 1
AHEAD = 2
LAG = 4
LEAD = 3
RATE = 2
BLOCK = 128
LANES = 128


def flipped(device, bit):
    return device + (1 - 2 * lax.rem(lax.div(device, bit), 2)) * bit


def mate(device, mask):
    bit = 1
    while bit <= mask:
        if mask & bit:
            device = flipped(device, bit)
        bit *= 2
    return device


def slot_of(device):
    return lax.div(device, 2 * PAIR) * PAIR + lax.rem(device, PAIR)


def gather_events(count):
    bits = []
    bit = count // 2
    while bit >= 1:
        if bit != PAIR:
            bits.append(bit)
        bit //= 2
    held, events = [0], []
    for bit in bits:
        events += [(bit, mask) for mask in held]
        held += [mask | bit for mask in held]
    return events


def span(index, size):
    return pl.ds(pl.multiple_of(index * size, size), size)


def window_kernel(
    sections, count,
    inputs, targets, gain_kept, lengths_kept, value_shard, output_shard, input_kept, output_kept,
    prior, queries_kept, scores,
    gain, lengths, input_map, output_map_small, queries, small_done,
    weights, work, strip, square, small, outer, inner, hidden, following, cotangent, previous, values, upstream, normed,
    activated, slopes, features, factors, gain_half, input_half, first_out, first_in,
    extra_own, extra_out, extra_in, staging, second_out, second_in, flats, everyone, rows_all, final,
    gather_send, gather_receive, own_weights, prior_done, staged, entry_own, entry_send, entry_receive,
    forward_send, forward_receive, backward_send, backward_receive,
    first_send, first_receive, extra_send, extra_receive, second_send, second_receive,
    publish_send, publish_receive, final_send, final_receive, turn,
):
    section, me = lax.axis_index("section"), lax.axis_index("dp")
    has_before, has_after = section > 0, section < sections - 1
    before, after = lax.max(section - 1, 0), lax.min(section + 1, sections - 1)
    side = lax.rem(lax.div(me, PAIR), 2)
    follows = lax.rem(section, 2) == 1
    leads = jnp.logical_not(follows)
    twin = section + 1 - 2 * lax.rem(section, 2)
    partner = flipped(me, PAIR)
    batches, example_length, width = inputs.shape
    entries, length = hidden.shape[0], hidden.shape[1]
    per_side = entries // 2
    cuts = per_side // batches
    half, value_width = weights.shape[1], weights.shape[2]
    rows = value_shard.shape[0]
    piece_rows = rows // PIECES
    stretch = PAIR * rows
    stretches = half // stretch
    size = work.shape[0]
    blocks = size // BLOCK
    feature_width = input_map.shape[0]
    signal_width = output_map_small.shape[0]
    chunks = forward_send.shape[1]
    chunk = half // chunks
    tiles = first_send.shape[1]
    tile = value_width // tiles
    group = 16
    shards = (value_shard, output_shard)
    value_map, output_map = weights.at[0], weights.at[1]
    events = gather_events(count)

    def gather_copy(number, array, piece, first):
        bit, mask = events[number]
        at = slot_of(mate(me, mask)) * PIECES + piece
        there = weights.at[array, span(at, piece_rows), :]
        here = shards[array].at[span(piece, piece_rows), :] if first else there
        return pltpu.make_async_remote_copy(
            src_ref=here,
            dst_ref=there,
            send_sem=gather_send.at[number, array, piece],
            recv_sem=gather_receive.at[number, array, piece],
            device_id={"dp": flipped(me, bit)},
            device_id_type=MESH,
        )

    def start_gather():
        for array in range(2):
            for piece in range(PIECES):
                for number, (_, mask) in enumerate(events):
                    if mask == 0:
                        gather_copy(number, array, piece, True).start()

    def serve(array, piece):
        for number, (bit, mask) in enumerate(events):
            forwards = [later for later, (_, want) in enumerate(events) if want == bit | mask]
            if forwards:
                gather_copy(number, array, piece, False).wait_recv()
            for later in forwards:
                gather_copy(later, array, piece, False).start()

    def collect(array):
        for number, (bit, mask) in enumerate(events):
            if all(want != bit | mask for _, want in events):
                @pl.loop(0, PIECES)
                def _(piece):
                    gather_copy(number, array, piece, False).wait_recv()

        kept[array].wait()

    def entry_copy(kind, entry, part, remote):
        source = (inputs, staging)[kind]
        sink = (hidden, cotangent)[kind]
        wanted = 1 - side if remote else side
        lines = pl.ds((entry % cuts) * length, length)
        here = source.at[entry // cuts, lines, span(2 * part + wanted, stretch)]
        there = sink.at[side * per_side + entry, :, span(part, stretch)]
        if not remote:
            return pltpu.make_async_copy(here, there, entry_own.at[kind, entry, part])
        return pltpu.make_async_remote_copy(
            src_ref=here,
            dst_ref=there,
            send_sem=entry_send.at[kind, entry, part],
            recv_sem=entry_receive.at[kind, entry, part],
            device_id={"dp": partner},
            device_id_type=MESH,
        )

    def entry_wait(kind, batch):
        sink = (hidden, cotangent)[kind]
        owner, entry = lax.div(batch, per_side), lax.rem(batch, per_side)
        for part in range(stretches):
            there = sink.at[batch, :, span(part, stretch)]

            @pl.when(owner == side)
            def _():
                pltpu.make_async_copy(there, there, entry_own.at[kind, entry, part]).wait()

            @pl.when(owner != side)
            def _():
                pltpu.make_async_remote_copy(
                    src_ref=there,
                    dst_ref=there,
                    send_sem=entry_send.at[kind, entry, part],
                    recv_sem=entry_receive.at[kind, entry, part],
                    device_id={"dp": partner},
                    device_id_type=MESH,
                ).wait_recv()

    def hop(source, sink, send, receive, device, batch, piece):
        columns = span(piece, chunk)
        return pltpu.make_async_remote_copy(
            src_ref=source.at[batch, :, columns],
            dst_ref=sink.at[batch, :, columns],
            send_sem=send.at[batch, piece],
            recv_sem=receive.at[batch, piece],
            device_id={"section": device},
            device_id_type=MESH,
        )

    def forward_copy(batch, piece):
        return hop(following, hidden, forward_send, forward_receive, after, batch, piece)

    def backward_copy(batch, piece):
        return hop(previous, cotangent, backward_send, backward_receive, before, batch, piece)

    def swap(source, sink, send, receive, batch, at):
        columns = span(at, tile)
        return pltpu.make_async_remote_copy(
            src_ref=source.at[batch, :, columns],
            dst_ref=sink.at[batch, :, columns],
            send_sem=send.at[batch, at],
            recv_sem=receive.at[batch, at],
            device_id={"dp": partner},
            device_id_type=MESH,
        )

    def first_copy(batch, at):
        return swap(first_out, first_in, first_send, first_receive, batch, at)

    def second_copy(batch, at):
        return swap(second_out, second_in, second_send, second_receive, batch, at)

    def extra_copy(batch):
        return pltpu.make_async_remote_copy(
            src_ref=extra_out.at[batch],
            dst_ref=extra_in.at[batch],
            send_sem=extra_send.at[batch],
            recv_sem=extra_receive.at[batch],
            device_id={"dp": partner},
            device_id_type=MESH,
        )

    small_copies = [
        pltpu.make_async_copy(source, sink, small_done.at[number])
        for number, (source, sink) in enumerate((
            (gain_kept, gain), (lengths_kept, lengths), (input_kept, input_map),
            (output_kept, output_map_small), (queries_kept, queries),
        ))
    ]
    for copy in small_copies:
        copy.start()
    prior_copy = pltpu.make_async_copy(prior, work, prior_done)
    prior_copy.start()
    stage_copy = pltpu.make_async_copy(targets, staging, staged)

    @pl.when(jnp.logical_not(has_after))
    def _():
        stage_copy.start()

    mine = span(slot_of(me), rows)
    kept = [
        pltpu.make_async_copy(shards[array], weights.at[array, mine, :], own_weights.at[array])
        for array in range(2)
    ]
    barrier = pltpu.get_barrier_semaphore()

    @pl.loop(1, count)
    def _(offset):
        pl.semaphore_signal(
            barrier, inc=1, device_id={"dp": lax.rem(me + offset, count)}, device_id_type=MESH
        )

    @pl.loop(1, sections)
    def _(offset):
        pl.semaphore_signal(
            barrier, inc=1, device_id={"section": lax.rem(section + offset, sections)},
            device_id_type=MESH,
        )

    pl.semaphore_wait(barrier, count + sections - 2)

    @pl.when(leads)
    def _():
        start_gather()

    def start_entries(kind):
        for entry in range(per_side):
            for part in range(stretches):
                entry_copy(kind, entry, part, True).start()
                entry_copy(kind, entry, part, False).start()

    @pl.when(jnp.logical_not(has_before))
    def _():
        start_entries(0)

    for copy in small_copies:
        copy.wait()

    @pl.when(jnp.logical_not(has_after))
    def _():
        stage_copy.wait()
        line = lax.broadcasted_iota(jnp.int32, (example_length, 1), 0)
        for entry in range(batches):
            live = jnp.where(line < lengths[:, entry : entry + 1], 1.0, 0.0)
            staging[entry] = staging[entry] * live.astype(jnp.bfloat16)

        start_entries(1)

    for copy in kept:
        copy.start()

    input_half[...] = jnp.zeros_like(input_half)
    for part in range(stretches):
        there = pl.ds(part * stretch, stretch)
        here = span(2 * part + side, stretch)
        gain_half[:, there] = gain[:, here].astype(jnp.float32)
        input_half[:feature_width, there] = input_map[:, here]
    for target, shift in ((outer, True), (inner, False)):
        entry = lax.broadcasted_iota(jnp.int32, target.shape, 1)
        line = lax.broadcasted_iota(jnp.int32, target.shape, 0)
        place = lax.div(entry, feature_width) if shift else lax.rem(entry, feature_width)
        target[...] = jnp.where(place == line, 1.0, 0.0).astype(jnp.bfloat16)
    prior_copy.wait()

    def forward_first(batch):
        @pl.when(jnp.logical_not(has_before))
        def _():
            entry_wait(0, batch)

        total = jnp.zeros((length, 1), jnp.float32)
        for piece in range(chunks):
            columns = pl.ds(piece * chunk, chunk)

            @pl.when(has_before)
            def _():
                forward_copy(batch, piece).wait_recv()

            widened = hidden[batch, :, columns].astype(jnp.float32)
            total = total + jnp.sum(widened * widened, axis=-1, keepdims=True)
            normed[:, columns] = (widened * gain_half[:, columns]).astype(jnp.bfloat16)

        for at in range(tiles):
            columns = pl.ds(at * tile, tile)
            found = jnp.dot(
                normed[...], value_map[:, columns], preferred_element_type=jnp.float32
            )
            values[batch, :, columns] = found
            first_out[batch, :, columns] = found.astype(jnp.bfloat16)
            first_copy(batch, at).start()
            if at == 0:
                extras = lax.dot_general(
                    normed[...], input_half[...], CONTRACT_LAST,
                    preferred_element_type=jnp.float32,
                )
                lanes = lax.broadcasted_iota(jnp.int32, extras.shape, 1)
                extra_own[batch] = jnp.where(lanes == feature_width, total, extras)
                high = total.astype(jnp.bfloat16).astype(jnp.float32)
                extras = jnp.where(lanes == feature_width, high, extras)
                extras = jnp.where(lanes == feature_width + 1, total - high, extras)
                extra_out[batch] = extras.astype(jnp.bfloat16)
                extra_copy(batch).start()

    def forward_second(batch):
        extra_copy(batch).wait_recv()
        arrived = extra_in[batch].astype(jnp.float32)
        both = extra_own[batch] + arrived
        total = (
            both[:, feature_width : feature_width + 1]
            + arrived[:, feature_width + 1 : feature_width + 2]
        )
        factor = lax.rsqrt(total * (1.0 / width) + 1e-05)
        factors[batch] = factor
        features[batch] = (both[:, :feature_width] * factor).astype(jnp.bfloat16)

        for at in range(tiles):
            columns = pl.ds(at * tile, tile)
            first_copy(batch, at).wait_recv()
            partial = first_in[batch, :, columns].astype(jnp.float32)
            found = (values[batch, :, columns] + partial) * factor
            values[batch, :, columns] = found
            activated[:, columns] = (found / (1.0 + jnp.exp(-found))).astype(jnp.bfloat16)

        @pl.when(has_after)
        def _():
            for piece in range(chunks):
                columns = pl.ds(piece * chunk, chunk)
                branch = lax.dot_general(
                    activated[...], output_map[columns, :], CONTRACT_LAST,
                    preferred_element_type=jnp.float32,
                )
                following[batch, :, columns] = (
                    hidden[batch, :, columns].astype(jnp.float32) + branch
                ).astype(jnp.bfloat16)
                forward_copy(batch, piece).start()

    def backward_first(batch):
        for at in range(tiles):
            columns = pl.ds(at * tile, tile)
            found = jnp.dot(
                cotangent[batch], output_map[:, columns], preferred_element_type=jnp.float32
            )
            upstream[batch, :, columns] = found
            second_out[batch, :, columns] = found.astype(jnp.bfloat16)
            second_copy(batch, at).start()

    def backward_second(batch):
        total = jnp.zeros((length, 1), jnp.float32)
        for at in range(tiles):
            columns = pl.ds(at * tile, tile)
            second_copy(batch, at).wait_recv()
            arrived = upstream[batch, :, columns] + second_in[batch, :, columns].astype(jnp.float32)
            found = values[batch, :, columns]
            logistic = 1.0 / (1.0 + jnp.exp(-found))
            slope = (arrived * logistic * (1.0 + found * (1.0 - logistic))).astype(jnp.bfloat16)
            slopes[:, columns] = slope
            total = total + jnp.sum(slope.astype(jnp.float32) * found, axis=-1, keepdims=True)

        factor = factors[batch]
        shrink = total * (factor * factor) * (1.0 / width)

        @pl.when(has_before)
        def _():
            for piece in range(chunks):
                columns = pl.ds(piece * chunk, chunk)
                normed_grad = lax.dot_general(
                    slopes[...], value_map[columns, :], CONTRACT_LAST,
                    preferred_element_type=jnp.float32,
                )
                weighted = normed_grad * gain_half[:, columns]
                hidden_grad = (
                    factor * weighted - hidden[batch, :, columns].astype(jnp.float32) * shrink
                )
                previous[batch, :, columns] = (
                    cotangent[batch, :, columns].astype(jnp.float32) + hidden_grad
                ).astype(jnp.bfloat16)
                backward_copy(batch, piece).start()

        signals = lax.dot_general(
            slopes[...], output_map_small[...], CONTRACT_LAST, preferred_element_type=jnp.float32
        ).astype(jnp.bfloat16)
        left = jnp.dot(signals, outer[...], preferred_element_type=jnp.float32)
        right = jnp.dot(features[batch], inner[...], preferred_element_type=jnp.float32)
        flat = jnp.sum(left * right, axis=0, keepdims=True) * (1.0 / example_length)
        flats[lax.div(batch, per_side), pl.ds(lax.rem(batch, per_side), 1), :] = flat

    def sweep(step):
        sweep_strip(work, strip, square, step, BLOCK)
        sweep_rest(work, strip, step, BLOCK)

    late = lax.rem(section, 2) * LAG
    served = pl.cdiv(LEAD + pl.cdiv(2 * PIECES, RATE), 2)
    stop = lax.min(late + served, blocks)

    def serve_at(point):
        for extra in range(RATE):
            number = point * RATE + extra

            @pl.when((number >= 0) & (number < 2 * PIECES))
            def _():
                bounded = lax.min(lax.max(number, 0), 2 * PIECES - 1)
                serve(lax.div(bounded, PIECES), lax.rem(bounded, PIECES))

    @pl.loop(0, late + served)
    def _(step):
        @pl.when(follows & (step == LAG))
        def _():
            pl.semaphore_wait(turn, 1)
            start_gather()

        point = 2 * (step - late) - LEAD

        @pl.when(step < blocks)
        def _():
            sweep_strip(work, strip, square, step, BLOCK)

        @pl.when((section == EAGER) & (step == late + served - 1))
        def _():
            collect(0)

            @pl.loop(0, AHEAD)
            def _(batch):
                forward_first(batch)

        serve_at(point)

        @pl.when(step < blocks)
        def _():
            sweep_rest(work, strip, step, BLOCK)

        serve_at(point + 1)

    @pl.when(section != EAGER)
    def _():
        collect(0)

    collect(1)

    @pl.when(leads)
    def _():
        pl.semaphore_signal(turn, inc=1, device_id={"section": twin}, device_id_type=MESH)

    first_stop = lax.select(has_before, blocks, stop)

    @pl.loop(stop, first_stop)
    def _(step):
        sweep(step)

    @pl.when(jnp.logical_not(has_after))
    def _():
        @pl.loop(0, entries)
        def _(batch):
            entry_wait(1, batch)
            backward_first(batch)

    @pl.loop(0, entries + 1)
    def _(batch):
        @pl.when((batch < entries) & ((section != EAGER) | (batch >= AHEAD)))
        def _():
            forward_first(lax.min(batch, entries - 1))

        @pl.when(batch > 0)
        def _():
            forward_second(lax.max(batch - 1, 0))

            @pl.when(jnp.logical_not(has_after))
            def _():
                backward_second(lax.max(batch - 1, 0))

    @pl.loop(first_stop, blocks)
    def _(step):
        sweep(step)

    @pl.when(has_after)
    def _():
        @pl.loop(0, entries + 1)
        def _(batch):
            @pl.when(batch < entries)
            def _():
                for piece in range(chunks):
                    backward_copy(lax.min(batch, entries - 1), piece).wait_recv()

                backward_first(lax.min(batch, entries - 1))

            @pl.when(batch > 0)
            def _():
                backward_second(lax.max(batch - 1, 0))

    ours = flats[side]
    for entry in range(batches):
        gathered = ours[entry * cuts : entry * cuts + 1, :]
        for cut in range(1, cuts):
            gathered = gathered + ours[entry * cuts + cut : entry * cuts + cut + 1, :]
        everyone[me, entry : entry + 1, :] = gathered

    def publish(offset, origin):
        return pltpu.make_async_remote_copy(
            src_ref=everyone.at[origin],
            dst_ref=everyone.at[origin],
            send_sem=publish_send.at[offset],
            recv_sem=publish_receive.at[offset],
            device_id={"dp": lax.rem(me + offset, count)},
            device_id_type=MESH,
        )

    @pl.loop(1, count)
    def _(offset):
        publish(offset, me).start()

    @pl.loop(1, count)
    def _(offset):
        publish(offset, lax.rem(me + count - offset, count)).wait_recv()

    for device in range(count):
        rows_all[device * batches : (device + 1) * batches, :] = everyone[device]
    grads = rows_all[...]
    examples = count * batches
    product = jnp.dot(grads, work[...], precision=HIGHEST, preferred_element_type=jnp.float32)
    gram = -lax.dot_general(
        product, grads, CONTRACT_LAST, precision=HIGHEST, preferred_element_type=jnp.float32
    )
    shape = (examples, examples)
    diagonal = lax.broadcasted_iota(jnp.int32, shape, 0) == lax.broadcasted_iota(jnp.int32, shape, 1)
    small[...] = jnp.zeros_like(small)
    small[:, :examples] = gram + jnp.where(diagonal, 1.0, 0.0)
    sweep_square(small)
    inverse = -small[:, :examples]
    picked = lax.broadcasted_iota(jnp.int32, (8, examples), 0)
    columns = lax.broadcasted_iota(jnp.int32, (8, examples), 1)
    pick = jnp.where((columns == me * batches + picked) & (picked < batches), 1.0, 0.0)
    owners = lax.broadcasted_iota(jnp.int32, (examples, queries.shape[1]), 0)
    selector = jnp.where(owners == queries[...], 1.0, 0.0)
    picked_gram = jnp.dot(pick, gram, precision=HIGHEST, preferred_element_type=jnp.float32)
    chosen = jnp.dot(inverse, selector, precision=HIGHEST, preferred_element_type=jnp.float32)
    final[section] = jnp.dot(picked_gram, chosen, precision=HIGHEST, preferred_element_type=jnp.float32)

    def finish(offset, origin):
        return pltpu.make_async_remote_copy(
            src_ref=final.at[origin],
            dst_ref=final.at[origin],
            send_sem=final_send.at[offset],
            recv_sem=final_receive.at[offset],
            device_id={"section": lax.rem(section + offset, sections)},
            device_id_type=MESH,
        )

    @pl.loop(1, sections)
    def _(offset):
        finish(offset, section).start()

    @pl.loop(1, sections)
    def _(offset):
        finish(offset, lax.rem(section + sections - offset, sections)).wait_recv()

    result = final[0]
    for other in range(1, sections):
        result = result + final[other]
    scores[...] = result[: scores.shape[0], : scores.shape[1]]

    @pl.loop(1, sections)
    def _(offset):
        finish(offset, section).wait_send()

    @pl.loop(1, count)
    def _(offset):
        publish(offset, me).wait_send()

    for kind, wanted in ((0, jnp.logical_not(has_before)), (1, jnp.logical_not(has_after))):
        @pl.when(wanted)
        def _():
            for entry in range(per_side):
                for part in range(stretches):
                    entry_copy(kind, entry, part, True).wait_send()

    for number, (_, mask) in enumerate(events):
        for array in range(2):
            @pl.loop(0, PIECES)
            def _(piece):
                gather_copy(number, array, piece, mask == 0).wait_send()

    @pl.loop(0, entries)
    def _(batch):
        extra_copy(batch).wait_send()

        @pl.loop(0, tiles)
        def _(at):
            first_copy(batch, at).wait_send()
            second_copy(batch, at).wait_send()

        @pl.loop(0, chunks)
        def _(piece):
            @pl.when(has_after)
            def _():
                forward_copy(batch, piece).wait_send()

            @pl.when(has_before)
            def _():
                backward_copy(batch, piece).wait_send()


def window(
    inputs, targets, gain, lengths, value_shard, output_shard, input_map, output_map_small, prior, queries
):
    sections, count = lax.axis_size("section"), lax.axis_size("dp")
    batches, example_length, width = inputs.shape
    rows, value_width = value_shard.shape
    cuts = 1
    length = example_length // cuts
    entries = 2 * batches * cuts
    half = width // 2
    size = prior.shape[0]
    feature_width = input_map.shape[0]
    signal_width = output_map_small.shape[0]
    asked = queries.shape[0]
    chunks, tiles = 4, 2
    events = len(gather_events(count))
    stretches = half // (PAIR * rows)
    dma = pltpu.SemaphoreType.DMA
    stream = pltpu.VMEM((entries, length, half), jnp.bfloat16)
    parts = pltpu.VMEM((entries, length, value_width), jnp.bfloat16)
    extra = pltpu.VMEM((entries, length, LANES), jnp.bfloat16)
    anywhere = pl.BlockSpec(memory_space=pl.ANY)
    inside = pl.BlockSpec(memory_space=pltpu.VMEM)
    return pl.pallas_call(
        functools.partial(window_kernel, sections, count),
        out_shape=jax.ShapeDtypeStruct((batches, asked), jnp.float32),
        in_specs=[
            anywhere, anywhere, anywhere, anywhere, anywhere, anywhere, anywhere, anywhere,
            anywhere, anywhere,
        ],
        out_specs=inside,
        scratch_shapes=[
            pltpu.VMEM(gain.shape, gain.dtype),
            pltpu.VMEM(lengths.shape, lengths.dtype),
            pltpu.VMEM(input_map.shape, input_map.dtype),
            pltpu.VMEM(output_map_small.shape, output_map_small.dtype),
            pltpu.VMEM((1, asked), queries.dtype),
            dma((5,)),
            pltpu.VMEM((2, half, value_width), jnp.bfloat16),
            pltpu.VMEM((size, size), jnp.float32),
            pltpu.VMEM((BLOCK, size), jnp.float32),
            pltpu.VMEM((BLOCK, BLOCK), jnp.float32),
            pltpu.VMEM((count * batches, LANES), jnp.float32),
            pltpu.VMEM((signal_width, size), jnp.bfloat16),
            pltpu.VMEM((feature_width, size), jnp.bfloat16),
            stream, stream, stream, stream,
            pltpu.VMEM((entries, length, value_width), jnp.float32),
            pltpu.VMEM((entries, length, value_width), jnp.float32),
            pltpu.VMEM((length, half), jnp.bfloat16),
            pltpu.VMEM((length, value_width), jnp.bfloat16),
            pltpu.VMEM((length, value_width), jnp.bfloat16),
            pltpu.VMEM((entries, length, feature_width), jnp.bfloat16),
            pltpu.VMEM((entries, length, 1), jnp.float32),
            pltpu.VMEM((1, half), jnp.float32),
            pltpu.VMEM((LANES, half), jnp.bfloat16),
            parts, parts, pltpu.VMEM((entries, length, LANES), jnp.float32), extra, extra,
            pltpu.VMEM((batches, example_length, width), jnp.bfloat16), parts, parts,
            pltpu.VMEM((2, batches * cuts, size), jnp.float32),
            pltpu.VMEM((count, batches, size), jnp.float32),
            pltpu.VMEM((count * batches, size), jnp.float32),
            pltpu.VMEM((sections, 8, asked), jnp.float32),
            dma((events, 2, PIECES)), dma((events, 2, PIECES)), dma((2,)), dma, dma,
            dma((2, batches * cuts, stretches)), dma((2, batches * cuts, stretches)),
            dma((2, batches * cuts, stretches)),
            dma((entries, chunks)), dma((entries, chunks)),
            dma((entries, chunks)), dma((entries, chunks)),
            dma((entries, tiles)), dma((entries, tiles)), dma((entries,)), dma((entries,)),
            dma((entries, tiles)), dma((entries, tiles)),
            dma((count,)), dma((count,)), dma((sections,)), dma((sections,)),
            pltpu.SemaphoreType.REGULAR,
        ],
        compiler_params=pltpu.CompilerParams(
            collective_id=1, has_side_effects=True, vmem_limit_bytes=67_000_000
        ),
        name="window",
    )(
        inputs, targets, gain, lengths, value_shard, output_shard, input_map, output_map_small,
        prior, queries[None, :],
    )


def per_device(
    inputs,
    output_cotangent,
    lengths,
    query_examples,
    norm_gain,
    value_weight,
    output_weight,
    input_projection,
    output_projection,
    fisher_prior,
):
    batches = lengths.shape[0]
    example_rows = inputs.shape[0] // batches
    width = inputs.shape[1]
    targets = output_cotangent.reshape(batches, example_rows, width)
    return window(
        inputs.reshape(batches, example_rows, width), targets, norm_gain, lengths[None, :],
        value_weight[0], output_weight[0], input_projection[0], output_projection[0],
        fisher_prior[0], query_examples,
    )


def solution(mesh):
    placed = (
        P("dp", None),
        P("dp", None),
        P("dp"),
        P(),
        P("section", None),
        P("section", "dp", None),
        P("section", "dp", None),
        P("section", None, None),
        P("section", None, None),
        P("section", None, None),
    )
    return jax.shard_map(
        per_device, mesh=mesh, in_specs=placed, out_specs=P("dp", None), check_vma=False
    )
```

```python
import functools

import jax
import jax.numpy as jnp
from jax import lax
from jax.experimental import pallas as pl
from jax.experimental.pallas import tpu as pltpu
from jax.sharding import PartitionSpec as P


HIGHEST = lax.Precision.HIGHEST


GROUP = 8


def small_inverse(held):
    count = len(held)
    held = [list(line) for line in held]
    for pivot in range(count):
        scale = 1.0 / held[pivot][pivot]
        line = list(held[pivot])
        scaled = [value * scale for value in line]
        for i in range(count):
            for j in range(i, count):
                if i != pivot and j != pivot:
                    held[i][j] = held[j][i] = held[i][j] - line[i] * scaled[j]
        for j in range(count):
            held[pivot][j] = held[j][pivot] = scaled[j]
        held[pivot][pivot] = -scale
    return [[-value for value in line] for line in held]


def sweep_square(square):
    rows, columns = square.shape
    lanes = lax.broadcasted_iota(jnp.int32, (GROUP, columns), 1)
    lines = lax.broadcasted_iota(jnp.int32, (GROUP, columns), 0)
    wide = lax.broadcasted_iota(jnp.int32, (rows, columns), 1)

    @pl.loop(0, rows // GROUP)
    def _(at):
        base = at * GROUP
        part = pl.ds(pl.multiple_of(base, GROUP), GROUP)
        panel = square[part, :]
        corner = [
            jnp.sum(jnp.where(lanes == base + k, panel, 0.0), axis=1, keepdims=True)
            for k in range(GROUP)
        ]
        spread = [
            [jnp.broadcast_to(corner[k][i : i + 1, :], (1, columns)) for k in range(GROUP)]
            for i in range(GROUP)
        ]
        inverse = small_inverse(spread)
        inside = (lanes >= base) & (lanes < base + GROUP)
        unit = jnp.where(lanes - base == lines, 1.0, 0.0)
        source = jnp.where(inside, unit, panel)
        built = []
        for i in range(GROUP):
            total = inverse[i][0] * source[:1, :]
            for k in range(1, GROUP):
                total = total + inverse[i][k] * source[k : k + 1, :]
            built.append(total)
        strip = jnp.concatenate(built, axis=0)
        signed = jnp.where(inside, -strip, strip)
        full = square[...]
        within = (wide >= base) & (wide < base + GROUP)
        updated = jnp.where(within, 0.0, full)
        for k in range(GROUP):
            column = jnp.sum(jnp.where(wide == base + k, full, 0.0), axis=1, keepdims=True)
            updated = updated - column * signed[k : k + 1, :]
        square[...] = updated
        square[part, :] = signed


def sweep_strip(work, strip, square, step, block):
    part = pl.ds(pl.multiple_of(step * block, block), block)
    square[...] = work[part, part]
    sweep_square(square)
    corner = square[...]
    strip[...] = -jnp.dot(
        corner, work[part, :], precision=HIGHEST, preferred_element_type=jnp.float32
    )
    strip[:, part] = corner


def sweep_rest(work, strip, step, block):
    span = pl.ds(pl.multiple_of(step * block, block), block)

    @pl.loop(0, work.shape[0] // block)
    def _(other):
        across = pl.ds(pl.multiple_of(other * block, block), block)

        @pl.when(other != step)
        def _():
            work[across, :] -= jnp.dot(
                work[span, across].T, strip[...], precision=HIGHEST,
                preferred_element_type=jnp.float32,
            )
            work[across, span] = strip[:, across].T

    work[span, :] = strip[...]


MESH = pl.DeviceIdType.MESH
CONTRACT_LAST = (((1,), (1,)), ((), ()))
PAIR = 2
PIECES = 4
TURN = 256
EAGER = 1
AHEAD = 2
LAG = 4
LEAD = 3
RATE = 2
BLOCK = 128
LANES = 128


def flipped(device, bit):
    return device + (1 - 2 * lax.rem(lax.div(device, bit), 2)) * bit


def mate(device, mask):
    bit = 1
    while bit <= mask:
        if mask & bit:
            device = flipped(device, bit)
        bit *= 2
    return device


def slot_of(device):
    return lax.div(device, 2 * PAIR) * PAIR + lax.rem(device, PAIR)


def gather_events(count):
    bits = []
    bit = count // 2
    while bit >= 1:
        if bit != PAIR:
            bits.append(bit)
        bit //= 2
    held, events = [0], []
    for bit in bits:
        events += [(bit, mask) for mask in held]
        held += [mask | bit for mask in held]
    return events


def span(index, size):
    return pl.ds(pl.multiple_of(index * size, size), size)


def window_kernel(
    sections, count,
    inputs, targets, gain_kept, lengths_kept, value_shard, output_shard, input_kept, output_kept,
    prior, queries_kept, scores,
    gain, lengths, input_map, output_map_small, queries, small_done,
    weights, turned, work, strip, square, small, outer, inner, hidden, following, cotangent, previous, values, upstream, normed,
    activated, slopes, features, factors, gain_half, input_half, first_out, first_in,
    extra_own, extra_out, extra_in, staging, second_out, second_in, flats, everyone, rows_all, final,
    gather_send, gather_receive, own_weights, prior_done, staged, entry_own, entry_send, entry_receive,
    forward_send, forward_receive, backward_send, backward_receive,
    first_send, first_receive, extra_send, extra_receive, second_send, second_receive,
    publish_send, publish_receive, final_send, final_receive, turn,
):
    section, me = lax.axis_index("section"), lax.axis_index("dp")
    has_before, has_after = section > 0, section < sections - 1
    before, after = lax.max(section - 1, 0), lax.min(section + 1, sections - 1)
    side = lax.rem(lax.div(me, PAIR), 2)
    follows = lax.rem(section, 2) == 1
    leads = jnp.logical_not(follows)
    twin = section + 1 - 2 * lax.rem(section, 2)
    partner = flipped(me, PAIR)
    batches, example_length, width = inputs.shape
    entries, length = hidden.shape[0], hidden.shape[1]
    per_side = entries // 2
    cuts = per_side // batches
    half, value_width = weights.shape[1], weights.shape[2]
    rows = value_shard.shape[0]
    piece_rows = rows // PIECES
    stretch = PAIR * rows
    stretches = half // stretch
    size = work.shape[0]
    blocks = size // BLOCK
    feature_width = input_map.shape[0]
    signal_width = output_map_small.shape[0]
    chunks = forward_send.shape[1]
    chunk = half // chunks
    tiles = first_send.shape[1]
    tile = value_width // tiles
    group = 16
    shards = (value_shard, output_shard)
    value_map, output_map = weights.at[0], weights.at[1]
    events = gather_events(count)

    def gather_copy(number, array, piece, first):
        bit, mask = events[number]
        at = slot_of(mate(me, mask)) * PIECES + piece
        there = weights.at[array, span(at, piece_rows), :]
        here = shards[array].at[span(piece, piece_rows), :] if first else there
        return pltpu.make_async_remote_copy(
            src_ref=here,
            dst_ref=there,
            send_sem=gather_send.at[number, array, piece],
            recv_sem=gather_receive.at[number, array, piece],
            device_id={"dp": flipped(me, bit)},
            device_id_type=MESH,
        )

    def start_gather():
        for array in range(2):
            for piece in range(PIECES):
                for number, (_, mask) in enumerate(events):
                    if mask == 0:
                        gather_copy(number, array, piece, True).start()

    def serve(array, piece):
        for number, (bit, mask) in enumerate(events):
            forwards = [later for later, (_, want) in enumerate(events) if want == bit | mask]
            if forwards:
                gather_copy(number, array, piece, False).wait_recv()
            for later in forwards:
                gather_copy(later, array, piece, False).start()

    def collect(array):
        for number, (bit, mask) in enumerate(events):
            if all(want != bit | mask for _, want in events):
                @pl.loop(0, PIECES)
                def _(piece):
                    gather_copy(number, array, piece, False).wait_recv()

        kept[array].wait()

    def entry_copy(kind, entry, part, remote):
        source = (inputs, staging)[kind]
        sink = (hidden, cotangent)[kind]
        wanted = 1 - side if remote else side
        lines = pl.ds((entry % cuts) * length, length)
        here = source.at[entry // cuts, lines, span(2 * part + wanted, stretch)]
        there = sink.at[side * per_side + entry, :, span(part, stretch)]
        if not remote:
            return pltpu.make_async_copy(here, there, entry_own.at[kind, entry, part])
        return pltpu.make_async_remote_copy(
            src_ref=here,
            dst_ref=there,
            send_sem=entry_send.at[kind, entry, part],
            recv_sem=entry_receive.at[kind, entry, part],
            device_id={"dp": partner},
            device_id_type=MESH,
        )

    def entry_wait(kind, batch):
        sink = (hidden, cotangent)[kind]
        owner, entry = lax.div(batch, per_side), lax.rem(batch, per_side)
        for part in range(stretches):
            there = sink.at[batch, :, span(part, stretch)]

            @pl.when(owner == side)
            def _():
                pltpu.make_async_copy(there, there, entry_own.at[kind, entry, part]).wait()

            @pl.when(owner != side)
            def _():
                pltpu.make_async_remote_copy(
                    src_ref=there,
                    dst_ref=there,
                    send_sem=entry_send.at[kind, entry, part],
                    recv_sem=entry_receive.at[kind, entry, part],
                    device_id={"dp": partner},
                    device_id_type=MESH,
                ).wait_recv()

    def hop(source, sink, send, receive, device, batch, piece):
        columns = span(piece, chunk)
        return pltpu.make_async_remote_copy(
            src_ref=source.at[batch, :, columns],
            dst_ref=sink.at[batch, :, columns],
            send_sem=send.at[batch, piece],
            recv_sem=receive.at[batch, piece],
            device_id={"section": device},
            device_id_type=MESH,
        )

    def forward_copy(batch, piece):
        return hop(following, hidden, forward_send, forward_receive, after, batch, piece)

    def backward_copy(batch, piece):
        return hop(previous, cotangent, backward_send, backward_receive, before, batch, piece)

    def swap(source, sink, send, receive, batch, at):
        columns = span(at, tile)
        return pltpu.make_async_remote_copy(
            src_ref=source.at[batch, :, columns],
            dst_ref=sink.at[batch, :, columns],
            send_sem=send.at[batch, at],
            recv_sem=receive.at[batch, at],
            device_id={"dp": partner},
            device_id_type=MESH,
        )

    def first_copy(batch, at):
        return swap(first_out, first_in, first_send, first_receive, batch, at)

    def second_copy(batch, at):
        return swap(second_out, second_in, second_send, second_receive, batch, at)

    def extra_copy(batch):
        return pltpu.make_async_remote_copy(
            src_ref=extra_out.at[batch],
            dst_ref=extra_in.at[batch],
            send_sem=extra_send.at[batch],
            recv_sem=extra_receive.at[batch],
            device_id={"dp": partner},
            device_id_type=MESH,
        )

    small_copies = [
        pltpu.make_async_copy(source, sink, small_done.at[number])
        for number, (source, sink) in enumerate((
            (gain_kept, gain), (lengths_kept, lengths), (input_kept, input_map),
            (output_kept, output_map_small), (queries_kept, queries),
        ))
    ]
    for copy in small_copies:
        copy.start()
    prior_copy = pltpu.make_async_copy(prior, work, prior_done)
    prior_copy.start()
    stage_copy = pltpu.make_async_copy(targets, staging, staged)

    @pl.when(jnp.logical_not(has_after))
    def _():
        stage_copy.start()

    mine = span(slot_of(me), rows)
    kept = [
        pltpu.make_async_copy(shards[array], weights.at[array, mine, :], own_weights.at[array])
        for array in range(2)
    ]
    barrier = pltpu.get_barrier_semaphore()

    @pl.loop(1, count)
    def _(offset):
        pl.semaphore_signal(
            barrier, inc=1, device_id={"dp": lax.rem(me + offset, count)}, device_id_type=MESH
        )

    @pl.loop(1, sections)
    def _(offset):
        pl.semaphore_signal(
            barrier, inc=1, device_id={"section": lax.rem(section + offset, sections)},
            device_id_type=MESH,
        )

    pl.semaphore_wait(barrier, count + sections - 2)

    @pl.when(leads)
    def _():
        start_gather()

    def start_entries(kind):
        for entry in range(per_side):
            for part in range(stretches):
                entry_copy(kind, entry, part, True).start()
                entry_copy(kind, entry, part, False).start()

    @pl.when(jnp.logical_not(has_before))
    def _():
        start_entries(0)

    for copy in small_copies:
        copy.wait()

    @pl.when(jnp.logical_not(has_after))
    def _():
        stage_copy.wait()
        line = lax.broadcasted_iota(jnp.int32, (example_length, 1), 0)
        for entry in range(batches):
            live = jnp.where(line < lengths[:, entry : entry + 1], 1.0, 0.0)
            staging[entry] = staging[entry] * live.astype(jnp.bfloat16)

        start_entries(1)

    for copy in kept:
        copy.start()

    input_half[...] = jnp.zeros_like(input_half)
    for part in range(stretches):
        there = pl.ds(part * stretch, stretch)
        here = span(2 * part + side, stretch)
        gain_half[:, there] = gain[:, here].astype(jnp.float32)
        input_half[:feature_width, there] = input_map[:, here]
    for target, shift in ((outer, True), (inner, False)):
        entry = lax.broadcasted_iota(jnp.int32, target.shape, 1)
        line = lax.broadcasted_iota(jnp.int32, target.shape, 0)
        place = lax.div(entry, feature_width) if shift else lax.rem(entry, feature_width)
        target[...] = jnp.where(place == line, 1.0, 0.0).astype(jnp.bfloat16)
    prior_copy.wait()

    def turn_over():
        @pl.loop(0, half // TURN)
        def _(at):
            part = span(at, TURN)
            turned[:, part] = value_map[part, :].T

    def forward_first(batch):
        @pl.when(jnp.logical_not(has_before))
        def _():
            entry_wait(0, batch)

        total = jnp.zeros((length, 1), jnp.float32)
        for piece in range(chunks):
            columns = pl.ds(piece * chunk, chunk)

            @pl.when(has_before)
            def _():
                forward_copy(batch, piece).wait_recv()

            widened = hidden[batch, :, columns].astype(jnp.float32)
            total = total + jnp.sum(widened * widened, axis=-1, keepdims=True)
            normed[:, columns] = (widened * gain_half[:, columns]).astype(jnp.bfloat16)

        for at in range(tiles):
            columns = pl.ds(at * tile, tile)
            found = jnp.dot(
                normed[...], value_map[:, columns], preferred_element_type=jnp.float32
            )
            values[batch, :, columns] = found
            first_out[batch, :, columns] = found.astype(jnp.bfloat16)
            first_copy(batch, at).start()
            if at == 0:
                extras = lax.dot_general(
                    normed[...], input_half[...], CONTRACT_LAST,
                    preferred_element_type=jnp.float32,
                )
                lanes = lax.broadcasted_iota(jnp.int32, extras.shape, 1)
                extra_own[batch] = jnp.where(lanes == feature_width, total, extras)
                high = total.astype(jnp.bfloat16).astype(jnp.float32)
                extras = jnp.where(lanes == feature_width, high, extras)
                extras = jnp.where(lanes == feature_width + 1, total - high, extras)
                extra_out[batch] = extras.astype(jnp.bfloat16)
                extra_copy(batch).start()

    def forward_second(batch):
        extra_copy(batch).wait_recv()
        arrived = extra_in[batch].astype(jnp.float32)
        both = extra_own[batch] + arrived
        total = (
            both[:, feature_width : feature_width + 1]
            + arrived[:, feature_width + 1 : feature_width + 2]
        )
        factor = lax.rsqrt(total * (1.0 / width) + 1e-05)
        factors[batch] = factor
        features[batch] = (both[:, :feature_width] * factor).astype(jnp.bfloat16)

        for at in range(tiles):
            columns = pl.ds(at * tile, tile)
            first_copy(batch, at).wait_recv()
            partial = first_in[batch, :, columns].astype(jnp.float32)
            found = (values[batch, :, columns] + partial) * factor
            values[batch, :, columns] = found
            activated[:, columns] = (found / (1.0 + jnp.exp(-found))).astype(jnp.bfloat16)

        @pl.when(has_after)
        def _():
            for piece in range(chunks):
                columns = pl.ds(piece * chunk, chunk)
                branch = lax.dot_general(
                    activated[...], output_map[columns, :], CONTRACT_LAST,
                    preferred_element_type=jnp.float32,
                )
                following[batch, :, columns] = (
                    hidden[batch, :, columns].astype(jnp.float32) + branch
                ).astype(jnp.bfloat16)
                forward_copy(batch, piece).start()

    def backward_first(batch):
        for at in range(tiles):
            columns = pl.ds(at * tile, tile)
            found = jnp.dot(
                cotangent[batch], output_map[:, columns], preferred_element_type=jnp.float32
            )
            upstream[batch, :, columns] = found
            second_out[batch, :, columns] = found.astype(jnp.bfloat16)
            second_copy(batch, at).start()

    def backward_second(batch):
        total = jnp.zeros((length, 1), jnp.float32)
        for at in range(tiles):
            columns = pl.ds(at * tile, tile)
            second_copy(batch, at).wait_recv()
            arrived = upstream[batch, :, columns] + second_in[batch, :, columns].astype(jnp.float32)
            found = values[batch, :, columns]
            logistic = 1.0 / (1.0 + jnp.exp(-found))
            slope = (arrived * logistic * (1.0 + found * (1.0 - logistic))).astype(jnp.bfloat16)
            slopes[:, columns] = slope
            total = total + jnp.sum(slope.astype(jnp.float32) * found, axis=-1, keepdims=True)

        factor = factors[batch]
        shrink = total * (factor * factor) * (1.0 / width)

        @pl.when(has_before)
        def _():
            for piece in range(chunks):
                columns = pl.ds(piece * chunk, chunk)
                normed_grad = jnp.dot(
                    slopes[...], turned[:, columns], preferred_element_type=jnp.float32
                )
                weighted = normed_grad * gain_half[:, columns]
                hidden_grad = (
                    factor * weighted - hidden[batch, :, columns].astype(jnp.float32) * shrink
                )
                previous[batch, :, columns] = (
                    cotangent[batch, :, columns].astype(jnp.float32) + hidden_grad
                ).astype(jnp.bfloat16)
                backward_copy(batch, piece).start()

        signals = lax.dot_general(
            slopes[...], output_map_small[...], CONTRACT_LAST, preferred_element_type=jnp.float32
        ).astype(jnp.bfloat16)
        left = jnp.dot(signals, outer[...], preferred_element_type=jnp.float32)
        right = jnp.dot(features[batch], inner[...], preferred_element_type=jnp.float32)
        flat = jnp.sum(left * right, axis=0, keepdims=True) * (1.0 / example_length)
        flats[lax.div(batch, per_side), pl.ds(lax.rem(batch, per_side), 1), :] = flat

    def sweep(step):
        sweep_strip(work, strip, square, step, BLOCK)
        sweep_rest(work, strip, step, BLOCK)

    late = lax.rem(section, 2) * LAG
    served = pl.cdiv(LEAD + pl.cdiv(2 * PIECES, RATE), 2)
    stop = lax.min(late + served, blocks)

    def serve_at(point):
        for extra in range(RATE):
            number = point * RATE + extra

            @pl.when((number >= 0) & (number < 2 * PIECES))
            def _():
                bounded = lax.min(lax.max(number, 0), 2 * PIECES - 1)
                serve(lax.div(bounded, PIECES), lax.rem(bounded, PIECES))

    @pl.loop(0, late + served)
    def _(step):
        @pl.when(follows & (step == LAG))
        def _():
            pl.semaphore_wait(turn, 1)
            start_gather()

        point = 2 * (step - late) - LEAD

        @pl.when(step < blocks)
        def _():
            sweep_strip(work, strip, square, step, BLOCK)

        @pl.when((section == EAGER) & (step == late + served - 1))
        def _():
            collect(0)

            @pl.loop(0, AHEAD)
            def _(batch):
                forward_first(batch)

        serve_at(point)

        @pl.when(step < blocks)
        def _():
            sweep_rest(work, strip, step, BLOCK)

        serve_at(point + 1)

    @pl.when(section != EAGER)
    def _():
        collect(0)

    collect(1)

    @pl.when(leads)
    def _():
        pl.semaphore_signal(turn, inc=1, device_id={"section": twin}, device_id_type=MESH)

    first_stop = lax.select(has_before, blocks, stop)

    @pl.loop(stop, first_stop)
    def _(step):
        sweep(step)

    @pl.when(section > EAGER)
    def _():
        turn_over()

    @pl.when(jnp.logical_not(has_after))
    def _():
        @pl.loop(0, entries)
        def _(batch):
            entry_wait(1, batch)
            backward_first(batch)

    @pl.loop(0, entries + 1)
    def _(batch):
        @pl.when((batch < entries) & ((section != EAGER) | (batch >= AHEAD)))
        def _():
            forward_first(lax.min(batch, entries - 1))

        @pl.when(batch > 0)
        def _():
            forward_second(lax.max(batch - 1, 0))

            @pl.when(jnp.logical_not(has_after))
            def _():
                backward_second(lax.max(batch - 1, 0))

    @pl.loop(first_stop, blocks)
    def _(step):
        sweep(step)

    @pl.when(section == EAGER)
    def _():
        turn_over()

    @pl.when(has_after)
    def _():
        @pl.loop(0, entries + 1)
        def _(batch):
            @pl.when(batch < entries)
            def _():
                for piece in range(chunks):
                    backward_copy(lax.min(batch, entries - 1), piece).wait_recv()

                backward_first(lax.min(batch, entries - 1))

            @pl.when(batch > 0)
            def _():
                backward_second(lax.max(batch - 1, 0))

    ours = flats[side]
    for entry in range(batches):
        gathered = ours[entry * cuts : entry * cuts + 1, :]
        for cut in range(1, cuts):
            gathered = gathered + ours[entry * cuts + cut : entry * cuts + cut + 1, :]
        everyone[me, entry : entry + 1, :] = gathered

    def publish(offset, origin):
        return pltpu.make_async_remote_copy(
            src_ref=everyone.at[origin],
            dst_ref=everyone.at[origin],
            send_sem=publish_send.at[offset],
            recv_sem=publish_receive.at[offset],
            device_id={"dp": lax.rem(me + offset, count)},
            device_id_type=MESH,
        )

    @pl.loop(1, count)
    def _(offset):
        publish(offset, me).start()

    @pl.loop(1, count)
    def _(offset):
        publish(offset, lax.rem(me + count - offset, count)).wait_recv()

    for device in range(count):
        rows_all[device * batches : (device + 1) * batches, :] = everyone[device]
    grads = rows_all[...]
    examples = count * batches
    product = jnp.dot(grads, work[...], precision=HIGHEST, preferred_element_type=jnp.float32)
    gram = -lax.dot_general(
        product, grads, CONTRACT_LAST, precision=HIGHEST, preferred_element_type=jnp.float32
    )
    shape = (examples, examples)
    diagonal = lax.broadcasted_iota(jnp.int32, shape, 0) == lax.broadcasted_iota(jnp.int32, shape, 1)
    small[...] = jnp.zeros_like(small)
    small[:, :examples] = gram + jnp.where(diagonal, 1.0, 0.0)
    sweep_square(small)
    inverse = -small[:, :examples]
    picked = lax.broadcasted_iota(jnp.int32, (8, examples), 0)
    columns = lax.broadcasted_iota(jnp.int32, (8, examples), 1)
    pick = jnp.where((columns == me * batches + picked) & (picked < batches), 1.0, 0.0)
    owners = lax.broadcasted_iota(jnp.int32, (examples, queries.shape[1]), 0)
    selector = jnp.where(owners == queries[...], 1.0, 0.0)
    picked_gram = jnp.dot(pick, gram, precision=HIGHEST, preferred_element_type=jnp.float32)
    chosen = jnp.dot(inverse, selector, precision=HIGHEST, preferred_element_type=jnp.float32)
    final[section] = jnp.dot(picked_gram, chosen, precision=HIGHEST, preferred_element_type=jnp.float32)

    def finish(offset, origin):
        return pltpu.make_async_remote_copy(
            src_ref=final.at[origin],
            dst_ref=final.at[origin],
            send_sem=final_send.at[offset],
            recv_sem=final_receive.at[offset],
            device_id={"section": lax.rem(section + offset, sections)},
            device_id_type=MESH,
        )

    @pl.loop(1, sections)
    def _(offset):
        finish(offset, section).start()

    @pl.loop(1, sections)
    def _(offset):
        finish(offset, lax.rem(section + sections - offset, sections)).wait_recv()

    result = final[0]
    for other in range(1, sections):
        result = result + final[other]
    scores[...] = result[: scores.shape[0], : scores.shape[1]]

    @pl.loop(1, sections)
    def _(offset):
        finish(offset, section).wait_send()

    @pl.loop(1, count)
    def _(offset):
        publish(offset, me).wait_send()

    for kind, wanted in ((0, jnp.logical_not(has_before)), (1, jnp.logical_not(has_after))):
        @pl.when(wanted)
        def _():
            for entry in range(per_side):
                for part in range(stretches):
                    entry_copy(kind, entry, part, True).wait_send()

    for number, (_, mask) in enumerate(events):
        for array in range(2):
            @pl.loop(0, PIECES)
            def _(piece):
                gather_copy(number, array, piece, mask == 0).wait_send()

    @pl.loop(0, entries)
    def _(batch):
        extra_copy(batch).wait_send()

        @pl.loop(0, tiles)
        def _(at):
            first_copy(batch, at).wait_send()
            second_copy(batch, at).wait_send()

        @pl.loop(0, chunks)
        def _(piece):
            @pl.when(has_after)
            def _():
                forward_copy(batch, piece).wait_send()

            @pl.when(has_before)
            def _():
                backward_copy(batch, piece).wait_send()


def window(
    inputs, targets, gain, lengths, value_shard, output_shard, input_map, output_map_small, prior, queries
):
    sections, count = lax.axis_size("section"), lax.axis_size("dp")
    batches, example_length, width = inputs.shape
    rows, value_width = value_shard.shape
    cuts = 1
    length = example_length // cuts
    entries = 2 * batches * cuts
    half = width // 2
    size = prior.shape[0]
    feature_width = input_map.shape[0]
    signal_width = output_map_small.shape[0]
    asked = queries.shape[0]
    chunks, tiles = 2, 4
    events = len(gather_events(count))
    stretches = half // (PAIR * rows)
    dma = pltpu.SemaphoreType.DMA
    stream = pltpu.VMEM((entries, length, half), jnp.bfloat16)
    parts = pltpu.VMEM((entries, length, value_width), jnp.bfloat16)
    extra = pltpu.VMEM((entries, length, LANES), jnp.bfloat16)
    anywhere = pl.BlockSpec(memory_space=pl.ANY)
    inside = pl.BlockSpec(memory_space=pltpu.VMEM)
    return pl.pallas_call(
        functools.partial(window_kernel, sections, count),
        out_shape=jax.ShapeDtypeStruct((batches, asked), jnp.float32),
        in_specs=[
            anywhere, anywhere, anywhere, anywhere, anywhere, anywhere, anywhere, anywhere,
            anywhere, anywhere,
        ],
        out_specs=inside,
        scratch_shapes=[
            pltpu.VMEM(gain.shape, gain.dtype),
            pltpu.VMEM(lengths.shape, lengths.dtype),
            pltpu.VMEM(input_map.shape, input_map.dtype),
            pltpu.VMEM(output_map_small.shape, output_map_small.dtype),
            pltpu.VMEM((1, asked), queries.dtype),
            dma((5,)),
            pltpu.VMEM((2, half, value_width), jnp.bfloat16),
            pltpu.VMEM((value_width, half), jnp.bfloat16),
            pltpu.VMEM((size, size), jnp.float32),
            pltpu.VMEM((BLOCK, size), jnp.float32),
            pltpu.VMEM((BLOCK, BLOCK), jnp.float32),
            pltpu.VMEM((count * batches, LANES), jnp.float32),
            pltpu.VMEM((signal_width, size), jnp.bfloat16),
            pltpu.VMEM((feature_width, size), jnp.bfloat16),
            stream, stream, stream, stream,
            pltpu.VMEM((entries, length, value_width), jnp.float32),
            pltpu.VMEM((entries, length, value_width), jnp.float32),
            pltpu.VMEM((length, half), jnp.bfloat16),
            pltpu.VMEM((length, value_width), jnp.bfloat16),
            pltpu.VMEM((length, value_width), jnp.bfloat16),
            pltpu.VMEM((entries, length, feature_width), jnp.bfloat16),
            pltpu.VMEM((entries, length, 1), jnp.float32),
            pltpu.VMEM((1, half), jnp.float32),
            pltpu.VMEM((LANES, half), jnp.bfloat16),
            parts, parts, pltpu.VMEM((entries, length, LANES), jnp.float32), extra, extra,
            pltpu.VMEM((batches, example_length, width), jnp.bfloat16), parts, parts,
            pltpu.VMEM((2, batches * cuts, size), jnp.float32),
            pltpu.VMEM((count, batches, size), jnp.float32),
            pltpu.VMEM((count * batches, size), jnp.float32),
            pltpu.VMEM((sections, 8, asked), jnp.float32),
            dma((events, 2, PIECES)), dma((events, 2, PIECES)), dma((2,)), dma, dma,
            dma((2, batches * cuts, stretches)), dma((2, batches * cuts, stretches)),
            dma((2, batches * cuts, stretches)),
            dma((entries, chunks)), dma((entries, chunks)),
            dma((entries, chunks)), dma((entries, chunks)),
            dma((entries, tiles)), dma((entries, tiles)), dma((entries,)), dma((entries,)),
            dma((entries, tiles)), dma((entries, tiles)),
            dma((count,)), dma((count,)), dma((sections,)), dma((sections,)),
            pltpu.SemaphoreType.REGULAR,
        ],
        compiler_params=pltpu.CompilerParams(
            collective_id=1, has_side_effects=True, vmem_limit_bytes=67_000_000
        ),
        name="window",
    )(
        inputs, targets, gain, lengths, value_shard, output_shard, input_map, output_map_small,
        prior, queries[None, :],
    )


def per_device(
    inputs,
    output_cotangent,
    lengths,
    query_examples,
    norm_gain,
    value_weight,
    output_weight,
    input_projection,
    output_projection,
    fisher_prior,
):
    batches = lengths.shape[0]
    example_rows = inputs.shape[0] // batches
    width = inputs.shape[1]
    targets = output_cotangent.reshape(batches, example_rows, width)
    return window(
        inputs.reshape(batches, example_rows, width), targets, norm_gain, lengths[None, :],
        value_weight[0], output_weight[0], input_projection[0], output_projection[0],
        fisher_prior[0], query_examples,
    )


def solution(mesh):
    placed = (
        P("dp", None),
        P("dp", None),
        P("dp"),
        P(),
        P("section", None),
        P("section", "dp", None),
        P("section", "dp", None),
        P("section", None, None),
        P("section", None, None),
        P("section", None, None),
    )
    return jax.shard_map(
        per_device, mesh=mesh, in_specs=placed, out_specs=P("dp", None), check_vma=False
    )
```
